128 devices in a mesh: rows: 8 (over z, core), model: 16 (over y, x).
Axes of the slice: x: 4, y: 4, z: 4, core: 2. Of those that a mesh axis runs over, the one named last changes fastest.
Arguments:
- train_query: bfloat16 [8192, 8192], P('rows', 'model'), may hold values from -0.0625 to 0.0625
- low_query: bfloat16 [8192, 16], P('rows'), may hold values from -0.0625 to 0.0625
- high_query: bfloat16 [16, 8192], P(None, 'model'), may hold values from -1.5 to 1.5
- train_key: bfloat16 [8192, 1024], P('rows', 'model'), may hold values from -0.0625 to 0.0625
- low_key: bfloat16 [8192, 16], P('rows'), may hold values from -0.0625 to 0.0625
- high_key: bfloat16 [16, 1024], P(None, 'model'), may hold values from -1.5 to 1.5
- train_value: bfloat16 [8192, 1024], P('rows', 'model'), may hold values from -0.0625 to 0.0625
- low_value: bfloat16 [8192, 16], P('rows'), may hold values from -0.0625 to 0.0625
- high_value: bfloat16 [16, 1024], P(None, 'model'), may hold values from -1.5 to 1.5
- train_mixed: bfloat16 [8192, 8192], P('model', 'rows'), may hold values from -0.0625 to 0.0625
- low_mixed: bfloat16 [8192, 16], P('model'), may hold values from -0.0625 to 0.0625
- high_mixed: bfloat16 [16, 8192], P(None, 'rows'), may hold values from -1.5 to 1.5
- norm_train: float32 [8192], P(('rows', 'model')), may hold values from 0.25 to 1.75
- norm_step: float32 [8192], P(('rows', 'model')), may hold values from -0.3 to 0.3
Outputs:
- serving_query: bfloat16 [8192, 8192], P('model')
- serving_key: bfloat16 [1024, 8192], P('model')
- serving_value: bfloat16 [1024, 8192], P('model')
- serving_mixed: bfloat16 [8192, 8192], P(None, 'model')
- serve_norm: bfloat16 [8192], replicated
The draws below stay inside these ranges and needn't reach their ends.
All inputs are finite; a program needn't handle non-finite values.
Results may differ from the reference program's by a relative error of at most 0.001.
Values may be sent and summed in bfloat16 or wider, within the bound.
A program may use at most 128 MiB of HBM per device.

```python
import jax
import jax.numpy as jnp

D_MODEL = 8192
Q_DIM = 8192
KV_DIM = 1024
RANK = 16


def level_of(key, dims, pieces, least, top_value):
    gain, own = 1.0, jax.random.fold_in(key, 6)
    for position, parts in pieces:
        heights = jnp.exp(jax.random.uniform(jax.random.fold_in(own, position), (parts,), jnp.float32, least / len(pieces), top_value / len(pieces)))
        gain = gain * jnp.repeat(heights, dims[position] // parts).reshape([-1 if axis == position else 1 for axis in range(len(dims))])
    return gain


def normal_values(stream_key, shape, width, limit, pieces=(), dtype=jnp.bfloat16):
    level = level_of(stream_key, shape, pieces, -0.22, 0.18) if pieces else 1.0
    values = jax.random.normal(stream_key, shape, jnp.float32) * width * level
    return jnp.minimum(jnp.maximum(values, -limit), limit).astype(dtype)


def setup_inputs(seed: int = 0) -> dict:
    key_of = jax.random.split(jax.random.key(seed), 15)
    train_query = normal_values(key_of[0], (D_MODEL, Q_DIM), D_MODEL ** -0.5, 0.0625, ((0, 8), (1, 16)))
    low_query = normal_values(key_of[1], (D_MODEL, RANK), D_MODEL ** -0.5, 0.0625, ((0, 8),))
    high_query = normal_values(key_of[2], (RANK, Q_DIM), RANK ** -0.5, 1.5, ((1, 16),))
    train_key = normal_values(key_of[3], (D_MODEL, KV_DIM), D_MODEL ** -0.5, 0.0625, ((0, 8), (1, 16)))
    low_key = normal_values(key_of[4], (D_MODEL, RANK), D_MODEL ** -0.5, 0.0625, ((0, 8),))
    high_key = normal_values(key_of[5], (RANK, KV_DIM), RANK ** -0.5, 1.5, ((1, 16),))
    train_value = normal_values(key_of[6], (D_MODEL, KV_DIM), D_MODEL ** -0.5, 0.0625, ((0, 8), (1, 16)))
    low_value = normal_values(key_of[7], (D_MODEL, RANK), D_MODEL ** -0.5, 0.0625, ((0, 8),))
    high_value = normal_values(key_of[8], (RANK, KV_DIM), RANK ** -0.5, 1.5, ((1, 16),))
    train_mixed = normal_values(key_of[9], (Q_DIM, D_MODEL), Q_DIM ** -0.5, 0.0625, ((0, 16), (1, 8)))
    low_mixed = normal_values(key_of[10], (Q_DIM, RANK), Q_DIM ** -0.5, 0.0625, ((0, 16),))
    high_mixed = normal_values(key_of[11], (RANK, D_MODEL), RANK ** -0.5, 1.5, ((1, 8),))
    norm_train = jnp.clip(1.0 + 0.15 * jax.random.normal(key_of[12], (D_MODEL,), jnp.float32), 0.25, 1.75)
    norm_step = jnp.clip(jax.random.uniform(key_of[13], (D_MODEL,), jnp.float32, -0.3, 0.3) * level_of(key_of[13], (D_MODEL,), ((0, 128),), -0.4, 0.0), -0.3, 0.3)
    return dict(train_query=train_query, low_query=low_query, high_query=high_query, train_key=train_key, low_key=low_key, high_key=high_key, train_value=train_value, low_value=low_value, high_value=high_value, train_mixed=train_mixed, low_mixed=low_mixed, high_mixed=high_mixed, norm_train=norm_train, norm_step=norm_step)


mix_rate = 0.5


def reference(train_query, low_query, high_query, train_key, low_key, high_key, train_value, low_value, high_value, train_mixed, low_mixed, high_mixed, norm_train, norm_step):
    whole_query = train_query.astype(jnp.float32) + mix_rate * jnp.dot(low_query, high_query, preferred_element_type=jnp.float32)
    whole_key = train_key.astype(jnp.float32) + mix_rate * jnp.dot(low_key, high_key, preferred_element_type=jnp.float32)
    whole_value = train_value.astype(jnp.float32) + mix_rate * jnp.dot(low_value, high_value, preferred_element_type=jnp.float32)
    whole_mixed = train_mixed.astype(jnp.float32) + mix_rate * jnp.dot(low_mixed, high_mixed, preferred_element_type=jnp.float32)
    serving_query = whole_query.T.astype(jnp.bfloat16)
    serving_key = whole_key.T.astype(jnp.bfloat16)
    serving_value = whole_value.T.astype(jnp.bfloat16)
    serving_mixed = whole_mixed.T.astype(jnp.bfloat16)
    serve_norm = (norm_train + norm_step).astype(jnp.bfloat16)
    return serving_query, serving_key, serving_value, serving_mixed, serve_norm
```

```python
import jax
import jax.numpy as jnp
from jax import lax
from jax.experimental import pallas as pl
from jax.experimental.pallas import tpu as pltpu
from jax.sharding import PartitionSpec as P

MESH = pl.DeviceIdType.MESH
HBM = pl.BlockSpec(memory_space=pltpu.HBM)
VMEM = pl.BlockSpec(memory_space=pltpu.VMEM)

mix_rate = 0.5

PIECES = 18
HALF = PIECES // 2


def comm_kernel(
    tq, tk, tv, tm, lq, hq, lk, hk, lv, hv, lm, hm, na, nb,
    b, nz,
    xq, xkv, xm, slq, shq, slk, shk, slv, shv, slm, shm, sna, snb, nx, ny,
    ld, send, near_a, near_b, far_a, far_b, part_send, part_recv,
    nx_send, nx_recv, ny_send, ny_recv, nz_send, nz_recv, np_send, np_recv,
):
    rows = lax.axis_index("rows")
    model = lax.axis_index("model")
    z, core = rows // 2, rows % 2
    y, x = model // 4, model % 4
    up, down = (z + 1) % 4, (z + 3) % 4
    far = (z + 2) % 4
    to_up = {"rows": up * 2 + core}
    to_down = {"rows": down * 2 + core}
    to_part = {"rows": z * 2 + 1 - core}
    to_x = [{"model": y * 4 + (x + d) % 4} for d in (1, 2, 3)]
    to_y = [{"model": ((y + d) % 4) * 4 + x} for d in (1, 2, 3)]

    loads = [
        (tk, xkv.at[pl.ds(0, 64)]), (tv, xkv.at[pl.ds(64, 64)]),
        (lk, slk), (hk, shk), (lv, slv), (hv, shv),
        (na, sna), (nb, snb),
        (lq, slq), (hq, shq), (tq, xq),
        (lm, slm), (hm, shm), (tm, xm),
    ]
    loads = [pltpu.make_async_copy(s, d, ld.at[i]) for i, (s, d) in enumerate(loads)]
    for c in loads:
        c.start()
    barrier = pltpu.get_barrier_semaphore()
    for peer in [to_up, to_down, to_part] + to_x + to_y:
        pl.semaphore_signal(barrier, inc=1, device_id=peer, device_id_type=MESH)

    def low_rank(high, low):
        return mix_rate * lax.dot_general(
            high, low, (((0,), (0,)), ((), ())), preferred_element_type=jnp.float32
        )

    for c in loads[:8]:
        c.wait()
    for j in range(2):
        cols = pl.ds(j * 512, 512)
        for k, (high, low) in enumerate(((shk, slk), (shv, slv))):
            half = pl.ds(k * 64, 64)
            b[rows, j, half, :] = (
                xkv[half, cols].astype(jnp.float32) + low_rank(high[...], low[:, cols])
            ).astype(jnp.bfloat16)
    gain = sna[...] + snb[...]
    nx[x] = jnp.concatenate([gain, gain], axis=1)

    def copy_to(src, index, send_sem, recv_sem, to):
        return pltpu.make_async_remote_copy(
            src_ref=b.at[src, index], dst_ref=b.at[src, index], send_sem=send_sem,
            recv_sem=recv_sem, device_id=to, device_id_type=MESH,
        )

    def send_own(k):
        copy_to(rows, k, send.at[0], near_a.at[k], to_up).start()
        copy_to(rows, k, send.at[1], near_b.at[k], to_down).start()

    def to_partner(chip, k):
        copy_to(chip * 2 + core, k, part_send.at[chip], part_recv.at[chip], to_part).start()

    pl.semaphore_wait(barrier, 9)
    send_own(0)
    send_own(1)

    nx_copies = [
        pltpu.make_async_remote_copy(
            src_ref=nx.at[x], dst_ref=nx.at[x], send_sem=nx_send.at[d], recv_sem=nx_recv.at[d],
            device_id=to, device_id_type=MESH,
        )
        for d, to in enumerate(to_x)
    ]
    for c in nx_copies:
        c.start()
    to_partner(z, 0)
    to_partner(z, 1)

    for c in loads[8:]:
        c.wait()

    def make_query(i):
        left, top = (i // 4) * 512, (i % 4) * 128
        left, top = pl.multiple_of(left, 512), pl.multiple_of(top, 128)
        part = low_rank(shq[:, pl.ds(top, 128)], slq[:, pl.ds(left, 512)])
        base = xq[pl.ds(left, 512), pl.ds(top, 128)].astype(jnp.float32)
        b[rows, 2 + i] = (base.T + part).astype(jnp.bfloat16)

    def make_mixed(i):
        top = pl.multiple_of(i * 128, 128)
        part = low_rank(shm[:, pl.ds(top, 128)], slm[...])
        base = xm[:, pl.ds(top, 128)].astype(jnp.float32)
        b[rows, 10 + i] = (base.T + part).astype(jnp.bfloat16)

    make_query(0)

    @pl.loop(1, 8)
    def _(i):
        make_query(i)
        send_own(1 + i)
        to_partner(z, 1 + i)

    make_mixed(0)
    send_own(9)
    to_partner(z, 9)

    @pl.loop(1, 8)
    def _(i):
        make_mixed(i)
        send_own(9 + i)
        to_partner(z, 9 + i)

    for c in nx_copies:
        c.wait()
    lane = lax.broadcasted_iota(jnp.int32, (1, 128), 1)
    ny[y, 0:1] = jnp.where(lane < 64, nx[0], nx[1])
    ny[y, 1:2] = jnp.where(lane < 64, nx[2], nx[3])
    send_own(17)
    to_partner(z, 17)
    ny_copies = [
        pltpu.make_async_remote_copy(
            src_ref=ny.at[y], dst_ref=ny.at[y], send_sem=ny_send.at[d], recv_sem=ny_recv.at[d],
            device_id=to, device_id_type=MESH,
        )
        for d, to in enumerate(to_y)
    ]
    for c in ny_copies:
        c.start()

    def near(first, last):
        @pl.loop(first, last)
        def _(j):
            a = 2 * j
            copy_to(down * 2 + core, a, send.at[0], near_a.at[a], to_up).wait_recv()
            copy_to(down * 2 + core, a, send.at[2], far_a.at[j], to_up).start()
            to_partner(down, a)
            copy_to(up * 2 + core, a, send.at[1], near_b.at[a], to_down).wait_recv()
            to_partner(up, a)
            c = 2 * j + 1
            copy_to(down * 2 + core, c, send.at[0], near_a.at[c], to_up).wait_recv()
            to_partner(down, c)
            copy_to(up * 2 + core, c, send.at[1], near_b.at[c], to_down).wait_recv()
            copy_to(up * 2 + core, c, send.at[3], far_b.at[j], to_down).start()
            to_partner(up, c)

    def nz_copy(src, send_sem, recv_sem, to):
        return pltpu.make_async_remote_copy(
            src_ref=nz.at[src], dst_ref=nz.at[src], send_sem=send_sem, recv_sem=recv_sem,
            device_id=to, device_id_type=MESH,
        )

    near(0, 2)
    for c in ny_copies:
        c.wait()
    for i in range(4):
        nz[rows, 2 * i : 2 * i + 2] = ny[i]
    near(2, 4)
    n_up = nz_copy(rows, nz_send.at[0], nz_recv.at[0], to_up)
    n_down = nz_copy(rows, nz_send.at[1], nz_recv.at[1], to_down)
    n_up.start()
    n_down.start()
    near(4, 6)
    n_up.wait()
    n_down.wait()
    n_far = nz_copy(down * 2 + core, nz_send.at[2], nz_recv.at[2], to_up)
    n_far.start()
    near(6, 8)
    n_far.wait()
    n_part = [nz_copy(c * 2 + core, np_send.at[c], np_recv.at[c], to_part) for c in range(4)]
    for c in n_part:
        c.start()
    near(8, 9)

    @pl.loop(0, HALF)
    def _(j):
        copy_to(far * 2 + core, 2 * j, send.at[2], far_a.at[j], to_up).wait_recv()
        to_partner(far, 2 * j)
        copy_to(far * 2 + core, 2 * j + 1, send.at[3], far_b.at[j], to_down).wait_recv()
        to_partner(far, 2 * j + 1)

    for c in n_part:
        c.wait()

    def all_of(src, count, send_sem, recv_sem, to):
        part = b.at[src, pl.ds(0, count)]
        return pltpu.make_async_remote_copy(
            src_ref=part, dst_ref=part, send_sem=send_sem, recv_sem=recv_sem,
            device_id=to, device_id_type=MESH,
        )

    all_of(rows, PIECES, send.at[0], near_a.at[0], to_up).wait_send()
    all_of(rows, PIECES, send.at[1], near_b.at[0], to_down).wait_send()
    all_of(rows, HALF, send.at[2], far_a.at[0], to_up).wait_send()
    all_of(rows, HALF, send.at[3], far_b.at[0], to_down).wait_send()
    for c in range(4):
        all_of(c * 2 + core, PIECES, part_send.at[c], part_recv.at[c], to_part).wait_send()
        all_of(c * 2 + 1 - core, PIECES, part_send.at[c], part_recv.at[c], to_part).wait_recv()


def comm(*args):
    bf16, f32 = jnp.bfloat16, jnp.float32
    dma = pltpu.SemaphoreType.DMA
    return pl.pallas_call(
        comm_kernel,
        out_shape=[pltpu.VMEM((8, PIECES, 128, 512), bf16), pltpu.VMEM((8, 8, 128), f32)],
        in_specs=[HBM] * len(args),
        out_specs=[VMEM] * 2,
        scratch_shapes=[
            pltpu.VMEM((1024, 512), bf16), pltpu.VMEM((128, 1024), bf16), pltpu.VMEM((512, 1024), bf16),
            pltpu.VMEM((16, 1024), bf16), pltpu.VMEM((16, 512), bf16),
            pltpu.VMEM((16, 1024), bf16), pltpu.VMEM((16, 64), bf16),
            pltpu.VMEM((16, 1024), bf16), pltpu.VMEM((16, 64), bf16),
            pltpu.VMEM((16, 512), bf16), pltpu.VMEM((16, 1024), bf16),
            pltpu.VMEM((1, 64), f32), pltpu.VMEM((1, 64), f32),
            pltpu.VMEM((4, 1, 128), f32), pltpu.VMEM((4, 2, 128), f32),
            dma((14,)), dma((4,)), dma((PIECES,)), dma((PIECES,)), dma((HALF,)), dma((HALF,)),
            dma((4,)), dma((4,)),
            dma((3,)), dma((3,)), dma((3,)), dma((3,)), dma((3,)), dma((3,)), dma((4,)), dma((4,)),
        ],
        compiler_params=pltpu.CompilerParams(
            collective_id=0, has_side_effects=True, vmem_limit_bytes=44 * 2**20
        ),
        name="comm",
    )(*args)


def write_kernel(b, nz, q, k, v, m, n, sem):
    for r in range(8):
        for j in range(2):
            cols = pl.ds(r * 1024 + j * 512, 512)
            pltpu.make_async_copy(b.at[r, j, pl.ds(0, 64)], k.at[:, cols], sem.at[0]).start()
            pltpu.make_async_copy(b.at[r, j, pl.ds(64, 64)], v.at[:, cols], sem.at[1]).start()

    @pl.loop(0, 8)
    def _(r):
        for i in range(8):
            pltpu.make_async_copy(
                b.at[r, 2 + i],
                q.at[pl.ds(i % 4 * 128, 128), pl.ds(pl.multiple_of(r * 1024 + i // 4 * 512, 512), 512)],
                sem.at[2],
            ).start()
            pltpu.make_async_copy(
                b.at[r, 10 + i], m.at[pl.ds(pl.multiple_of(r * 1024 + i * 128, 128), 128)], sem.at[3]
            ).start()

    n[...] = nz[...].reshape(64, 128).astype(jnp.bfloat16)
    for i, ref in enumerate((k, v, q, m)):
        pltpu.make_async_copy(ref, ref, sem.at[i]).wait()


def write(b, nz):
    bf16 = jnp.bfloat16
    shapes = [(512, 8192), (64, 8192), (64, 8192), (8192, 512), (64, 128)]
    return pl.pallas_call(
        write_kernel,
        out_shape=[jax.ShapeDtypeStruct(s, bf16) for s in shapes],
        in_specs=[VMEM] * 2,
        out_specs=[HBM] * 4 + [VMEM],
        scratch_shapes=[pltpu.SemaphoreType.DMA((4,))],
        compiler_params=pltpu.CompilerParams(vmem_limit_bytes=4 * 2**20),
        name="write",
    )(b, nz)


def body(
    train_query, low_query, high_query, train_key, low_key, high_key, train_value, low_value, high_value,
    train_mixed, low_mixed, high_mixed, norm_train, norm_step,
):
    b, nz = comm(
        train_query, train_key.T, train_value.T, train_mixed,
        low_query.T, high_query, low_key.T, high_key, low_value.T, high_value, low_mixed.T, high_mixed,
        norm_train.reshape(1, 64), norm_step.reshape(1, 64),
    )
    q, k, v, m, n = write(b, nz)
    return q, k, v, m, n.reshape(8192)


def solution(mesh):
    R, M = "rows", "model"
    return jax.shard_map(
        body,
        mesh=mesh,
        in_specs=(
            P(R, M), P(R, None), P(None, M),
            P(R, M), P(R, None), P(None, M),
            P(R, M), P(R, None), P(None, M),
            P(M, R), P(M, None), P(None, R),
            P((R, M)), P((R, M)),
        ),
        out_specs=(P(M, None), P(M, None), P(M, None), P(None, M), P()),
        check_vma=False,
    )
```

```python
import jax
import jax.numpy as jnp
from jax import lax
from jax.experimental import pallas as pl
from jax.experimental.pallas import tpu as pltpu
from jax.sharding import PartitionSpec as P

MESH = pl.DeviceIdType.MESH
HBM = pl.BlockSpec(memory_space=pltpu.HBM)
VMEM = pl.BlockSpec(memory_space=pltpu.VMEM)

mix_rate = 0.5

PIECES = 18
HALF = PIECES // 2


def comm_kernel(
    tq, tk, tv, tm, lq, hq, lk, hk, lv, hv, lm, hm, na, nb,
    b, nz,
    xq, xk, xv, xm, slq, shq, slk, shk, slv, shv, slm, shm, sna, snb, gz, gx, gy,
    ld, send, near_a, near_b, far_a, far_b, part_send, part_recv,
    gz_send, gz_recv, gx_send, gx_recv, gy_send, gy_recv, nz_send, nz_recv,
):
    rows = lax.axis_index("rows")
    model = lax.axis_index("model")
    z, core = rows // 2, rows % 2
    y, x = model // 4, model % 4
    up, down = (z + 1) % 4, (z + 3) % 4
    far = (z + 2) % 4
    right, left, above, below = (x + 1) % 4, (x + 3) % 4, (y + 1) % 4, (y + 3) % 4
    to_up = {"rows": up * 2 + core}
    to_down = {"rows": down * 2 + core}
    to_part = {"rows": z * 2 + 1 - core}
    to_far, to_zero = {"rows": far * 2 + core}, {"rows": core}
    to_right, to_left = {"model": y * 4 + right}, {"model": y * 4 + left}
    to_above, to_below = {"model": above * 4 + x}, {"model": below * 4 + x}

    barrier = pltpu.get_barrier_semaphore()
    for peer in (to_up, to_down, to_part):
        pl.semaphore_signal(barrier, inc=1, device_id=peer, device_id_type=MESH)

    @pl.when(z == 0)
    def _():
        for peer in (to_far, to_right, to_left, to_above, to_below):
            pl.semaphore_signal(barrier, inc=1, device_id=peer, device_id_type=MESH)

    @pl.when(z == 2)
    def _():
        pl.semaphore_signal(barrier, inc=1, device_id=to_far, device_id_type=MESH)

    loads = [
        (na, sna), (nb, snb), (tk, xk), (lk, slk), (hk, shk), (tv, xv), (lv, slv), (hv, shv),
        (lm, slm), (hm, shm), (tm, xm),
        (lq, slq), (hq, shq), (tq, xq),
    ]
    loads = [pltpu.make_async_copy(s, d, ld.at[i]) for i, (s, d) in enumerate(loads)]
    for c in loads:
        c.start()

    def low_rank(high, low):
        return mix_rate * lax.dot_general(
            high, low, (((0,), (0,)), ((), ())), preferred_element_type=jnp.float32
        )

    def make_narrow(k, base, high, low):
        for j in range(2):
            cols = pl.ds(j * 512, 512)
            b[rows, k, pl.ds(j * 64, 64), :] = (
                base[:, cols].astype(jnp.float32) + low_rank(high[...], low[:, cols])
            ).astype(jnp.bfloat16)

    def copy_to(src, index, send_sem, recv_sem, to):
        return pltpu.make_async_remote_copy(
            src_ref=b.at[src, index], dst_ref=b.at[src, index], send_sem=send_sem,
            recv_sem=recv_sem, device_id=to, device_id_type=MESH,
        )

    def gz_copy(chip, to):
        return pltpu.make_async_remote_copy(
            src_ref=gz.at[chip], dst_ref=gz.at[chip], send_sem=gz_send, recv_sem=gz_recv.at[chip],
            device_id=to, device_id_type=MESH,
        )

    def send_own(k):
        copy_to(rows, k, send.at[0], near_a.at[k], to_up).start()
        copy_to(rows, k, send.at[1], near_b.at[k], to_down).start()

    def to_partner(chip, k):
        copy_to(chip * 2 + core, k, part_send.at[chip], part_recv.at[chip], to_part).start()

    for c in loads[:5]:
        c.wait()
    gain = sna[...] + snb[...]
    gz[z] = jnp.concatenate([gain, gain], axis=1)
    make_narrow(0, xk, shk, slk)
    pl.when(z == 0)(lambda: pl.semaphore_wait(barrier, 8))
    pl.when(z == 2)(lambda: pl.semaphore_wait(barrier, 4))
    pl.when(z % 2 == 1)(lambda: pl.semaphore_wait(barrier, 3))

    @pl.when(z != 0)
    def _():
        gz_copy(z, to_zero).start()

    for c in loads[5:8]:
        c.wait()
    send_own(0)
    make_narrow(1, xv, shv, slv)
    for c in loads[8:]:
        c.wait()
    send_own(1)
    to_partner(z, 0)
    to_partner(z, 1)

    def make_query(i):
        left, top = (i // 4) * 512, (i % 4) * 128
        left, top = pl.multiple_of(left, 512), pl.multiple_of(top, 128)
        part = low_rank(shq[:, pl.ds(top, 128)], slq[:, pl.ds(left, 512)])
        base = xq[pl.ds(left, 512), pl.ds(top, 128)].astype(jnp.float32)
        b[rows, 2 + i] = (base.T + part).astype(jnp.bfloat16)

    def make_mixed(i):
        top = pl.multiple_of(i * 128, 128)
        part = low_rank(shm[:, pl.ds(top, 128)], slm[...])
        base = xm[:, pl.ds(top, 128)].astype(jnp.float32)
        b[rows, 10 + i] = (base.T + part).astype(jnp.bfloat16)

    make_query(0)

    @pl.loop(1, 8)
    def _(i):
        make_query(i)
        send_own(1 + i)
        to_partner(z, 1 + i)

    make_mixed(0)
    send_own(9)
    to_partner(z, 9)

    @pl.loop(1, 8)
    def _(i):
        make_mixed(i)
        send_own(9 + i)
        to_partner(z, 9 + i)

    def tile(ref, src, sems, k, to):
        return pltpu.make_async_remote_copy(
            src_ref=ref.at[src], dst_ref=ref.at[src], send_sem=sems[0].at[k], recv_sem=sems[1].at[k],
            device_id=to, device_id_type=MESH,
        )

    def both(ref, src, sems, one, other):
        return [tile(ref, src, sems, 0, one), tile(ref, src, sems, 1, other)]

    gx_sems, gy_sems, nz_sems = (gx_send, gx_recv), (gy_send, gy_recv), (nz_send, nz_recv)
    gx_near, gx_far = both(gx, x, gx_sems, to_right, to_left), tile(gx, left, gx_sems, 2, to_right)
    gy_near, gy_far = both(gy, y, gy_sems, to_above, to_below), tile(gy, below, gy_sems, 2, to_above)
    nz_part = tile(nz, core, nz_sems, 3, to_part)

    def nz_back(chip):
        return pltpu.make_async_remote_copy(
            src_ref=nz.at[core], dst_ref=nz.at[core], send_sem=nz_send.at[chip - 1], recv_sem=nz_recv.at[0],
            device_id={"rows": chip * 2 + core}, device_id_type=MESH,
        )

    def make_x():
        for i in range(1, 4):
            gz_copy(i, to_up).wait_recv()
        for i in range(4):
            gx[x, i : i + 1] = gz[i]

    def near_x():
        for c in gx_near:
            c.start()

    def far_x():
        for c in gx_near:
            c.wait()
        gx_far.start()

    def make_y():
        gx_far.wait()
        lane = lax.broadcasted_iota(jnp.int32, (4, 128), 1)
        gy[y, 0] = jnp.where(lane < 64, gx[0], gx[1])
        gy[y, 1] = jnp.where(lane < 64, gx[2], gx[3])

    def near_y():
        for c in gy_near:
            c.start()

    def far_y():
        for c in gy_near:
            c.wait()
        gy_far.start()

    def make_z():
        gy_far.wait()
        for i in range(4):
            for k in range(8):
                nz[core, i, k : k + 1] = gy[k // 2, k % 2, i : i + 1]

    def back_z():
        for i in range(1, 4):
            nz_back(i).start()

    gain_steps = [near_x, far_x, make_y, near_y, far_y, make_z, back_z]
    pl.when(z == 0)(make_x)
    send_own(17)
    to_partner(z, 17)

    def fourth(src, index, i, send_sem, recv_sem, to):
        part = b.at[src, index, pl.ds(i * 32, 32)]
        return pltpu.make_async_remote_copy(
            src_ref=part, dst_ref=part, send_sem=send_sem, recv_sem=recv_sem, device_id=to, device_id_type=MESH
        )

    def pass_on(src, j, send_sem, sems, to, index):
        if j < HALF - 1:
            copy_to(src, index, send_sem, sems.at[j], to).start()
        else:
            for i in range(4):
                fourth(src, index, i, send_sem, sems.at[j + i], to).start()

    below_chip, above_chip = down * 2 + core, up * 2 + core
    for k in range(PIECES):
        j = k // 2
        copy_to(below_chip, k, send.at[0], near_a.at[k], to_up).wait_recv()
        if k % 2 == 0:
            pass_on(below_chip, j, send.at[2], far_a, to_up, k)
        to_partner(down, k)
        copy_to(above_chip, k, send.at[1], near_b.at[k], to_down).wait_recv()
        if k % 2 == 1:
            pass_on(above_chip, j, send.at[3], far_b, to_down, k)
        to_partner(up, k)
        if k < len(gain_steps):
            pl.when(z == 0)(gain_steps[k])

    far_chip = far * 2 + core

    def far_pieces(first, last):
        @pl.loop(first, last)
        def _(j):
            copy_to(far_chip, 2 * j, send.at[2], far_a.at[j], to_up).wait_recv()
            to_partner(far, 2 * j)
            copy_to(far_chip, 2 * j + 1, send.at[3], far_b.at[j], to_down).wait_recv()
            to_partner(far, 2 * j + 1)

    far_pieces(0, 5)

    @pl.when(z != 0)
    def _():
        gz_copy(z, to_zero).wait_send()
        nz_back(1).wait_recv()

    @pl.when(z == 0)
    def _():
        for i in range(1, 4):
            nz_back(i).wait_send()

    nz_part.start()
    far_pieces(5, HALF - 1)
    nz_part.wait()

    def all_of(src, count, send_sem, recv_sem, to):
        part = b.at[src, pl.ds(0, count)]
        return pltpu.make_async_remote_copy(
            src_ref=part, dst_ref=part, send_sem=send_sem, recv_sem=recv_sem,
            device_id=to, device_id_type=MESH,
        )

    for i in range(4):
        for index, sems, sem, to in ((16, far_a, send.at[2], to_up), (17, far_b, send.at[3], to_down)):
            fourth(far_chip, index, i, sem, sems.at[HALF - 1 + i], to).wait_recv()
            fourth(far_chip, index, i, part_send.at[far], part_recv.at[far], to_part).start()

    all_of(rows, PIECES, send.at[0], near_a.at[0], to_up).wait_send()
    all_of(rows, PIECES, send.at[1], near_b.at[0], to_down).wait_send()
    all_of(rows, HALF, send.at[2], far_a.at[0], to_up).wait_send()
    all_of(rows, HALF, send.at[3], far_b.at[0], to_down).wait_send()
    for c in range(4):
        all_of(c * 2 + core, PIECES, part_send.at[c], part_recv.at[c], to_part).wait_send()
        all_of(c * 2 + 1 - core, PIECES, part_send.at[c], part_recv.at[c], to_part).wait_recv()


def comm(*args):
    bf16, f32 = jnp.bfloat16, jnp.float32
    dma = pltpu.SemaphoreType.DMA
    return pl.pallas_call(
        comm_kernel,
        out_shape=[pltpu.VMEM((8, PIECES, 128, 512), bf16), pltpu.VMEM((2, 4, 8, 128), f32)],
        in_specs=[HBM] * len(args),
        out_specs=[VMEM] * 2,
        scratch_shapes=[
            pltpu.VMEM((1024, 512), bf16), pltpu.VMEM((64, 1024), bf16), pltpu.VMEM((64, 1024), bf16),
            pltpu.VMEM((512, 1024), bf16),
            pltpu.VMEM((16, 1024), bf16), pltpu.VMEM((16, 512), bf16),
            pltpu.VMEM((16, 1024), bf16), pltpu.VMEM((16, 64), bf16),
            pltpu.VMEM((16, 1024), bf16), pltpu.VMEM((16, 64), bf16),
            pltpu.VMEM((16, 512), bf16), pltpu.VMEM((16, 1024), bf16),
            pltpu.VMEM((1, 64), f32), pltpu.VMEM((1, 64), f32),
            pltpu.VMEM((4, 1, 128), f32), pltpu.VMEM((4, 4, 128), f32), pltpu.VMEM((4, 2, 4, 128), f32),
            dma((14,)), dma((4,)), dma((PIECES,)), dma((PIECES,)), dma((HALF + 3,)), dma((HALF + 3,)),
            dma((4,)), dma((4,)),
            dma, dma((4,)), dma((3,)), dma((3,)), dma((3,)), dma((3,)), dma((4,)), dma((4,)),
        ],
        compiler_params=pltpu.CompilerParams(
            collective_id=0, has_side_effects=True, vmem_limit_bytes=44 * 2**20
        ),
        name="comm",
    )(*args)


def write_kernel(b, nz, q, k, v, m, n, gain, sem):
    tiles = [nz[r % 2, r // 2] for r in range(8)]
    gain[...] = jnp.concatenate(tiles, axis=0).astype(jnp.bfloat16)
    for r in range(8):
        for j in range(2):
            cols, half = pl.ds(r * 1024 + j * 512, 512), pl.ds(j * 64, 64)
            pltpu.make_async_copy(b.at[r, 0, half], k.at[:, cols], sem.at[0]).start()
            pltpu.make_async_copy(b.at[r, 1, half], v.at[:, cols], sem.at[1]).start()
    for r in range(8):
        pltpu.make_async_copy(b.at[r, pl.ds(10, 8)], m.at[pl.ds(r * 8, 8)], sem.at[3]).start()
        for j in range(2):
            cols = pl.ds(r * 1024 + j * 512, 512)
            pltpu.make_async_copy(b.at[r, pl.ds(2 + 4 * j, 4)], q.at[:, :, cols], sem.at[2]).start()
    pltpu.make_async_copy(gain, n, sem.at[4]).start()
    for i, ref in enumerate((k, v, q, m, n)):
        pltpu.make_async_copy(ref, ref, sem.at[i]).wait()


def write(b, nz):
    bf16 = jnp.bfloat16
    shapes = [(4, 128, 8192), (64, 8192), (64, 8192), (64, 128, 512), (64, 128)]
    return pl.pallas_call(
        write_kernel,
        out_shape=[jax.ShapeDtypeStruct(s, bf16) for s in shapes],
        in_specs=[VMEM] * 2,
        out_specs=[HBM] * 5,
        scratch_shapes=[pltpu.VMEM((64, 128), bf16), pltpu.SemaphoreType.DMA((5,))],
        compiler_params=pltpu.CompilerParams(vmem_limit_bytes=4 * 2**20),
        name="write",
    )(b, nz)


def body(
    train_query, low_query, high_query, train_key, low_key, high_key, train_value, low_value, high_value,
    train_mixed, low_mixed, high_mixed, norm_train, norm_step,
):
    b, nz = comm(
        train_query, train_key.T, train_value.T, train_mixed,
        low_query.T, high_query, low_key.T, high_key, low_value.T, high_value, low_mixed.T, high_mixed,
        norm_train.reshape(1, 64), norm_step.reshape(1, 64),
    )
    q, k, v, m, n = write(b, nz)
    return q.reshape(512, 8192), k, v, m.reshape(8192, 512), n.reshape(8192)


def solution(mesh):
    R, M = "rows", "model"
    return jax.shard_map(
        body,
        mesh=mesh,
        in_specs=(
            P(R, M), P(R, None), P(None, M),
            P(R, M), P(R, None), P(None, M),
            P(R, M), P(R, None), P(None, M),
            P(M, R), P(M, None), P(None, R),
            P((R, M)), P((R, M)),
        ),
        out_specs=(P(M, None), P(M, None), P(M, None), P(None, M), P()),
        check_vma=False,
    )
```

```python
import jax
import jax.numpy as jnp
from jax import lax
from jax.experimental import pallas as pl
from jax.experimental.pallas import tpu as pltpu
from jax.sharding import PartitionSpec as P

MESH = pl.DeviceIdType.MESH
HBM = pl.BlockSpec(memory_space=pltpu.HBM)
VMEM = pl.BlockSpec(memory_space=pltpu.VMEM)

mix_rate = 0.5

PIECES = 18

SPLIT = 96
WAY_UP = ((0, 0, SPLIT),)
WAY_DOWN = ((0, SPLIT, 128 - SPLIT), (1, 0, 128)) if SPLIT < 128 else ((1, 0, 128),)


def comm_kernel(
    tq, tk, tv, tm, lq, hq, lk, hk, lv, hv, lm, hm, na, nb,
    b, late, nz,
    xq, xk, xv, xm, slq, shq, slk, shk, slv, shv, slm, shm, sna, snb, gz, gx, gy,
    ld, send, near_a, near_b, far_a, far_b, part_send, part_recv,
    gz_send, gz_recv, gx_send, gx_recv, gy_send, gy_recv, nz_send, nz_recv,
    late_send, late_recv,
):
    rows = lax.axis_index("rows")
    model = lax.axis_index("model")
    z, core = rows // 2, rows % 2
    y, x = model // 4, model % 4
    up, down = (z + 1) % 4, (z + 3) % 4
    far = (z + 2) % 4
    right, left, above, below = (x + 1) % 4, (x + 3) % 4, (y + 1) % 4, (y + 3) % 4
    to_up = {"rows": up * 2 + core}
    to_down = {"rows": down * 2 + core}
    to_part = {"rows": z * 2 + 1 - core}
    to_far, to_zero = {"rows": far * 2 + core}, {"rows": core}
    to_right, to_left = {"model": y * 4 + right}, {"model": y * 4 + left}
    to_above, to_below = {"model": above * 4 + x}, {"model": below * 4 + x}

    barrier = pltpu.get_barrier_semaphore()
    for peer in (to_up, to_down, to_part):
        pl.semaphore_signal(barrier, inc=1, device_id=peer, device_id_type=MESH)

    @pl.when(z == 0)
    def _():
        for peer in (to_far, to_right, to_left, to_above, to_below):
            pl.semaphore_signal(barrier, inc=1, device_id=peer, device_id_type=MESH)

    @pl.when(z == 2)
    def _():
        pl.semaphore_signal(barrier, inc=1, device_id=to_far, device_id_type=MESH)

    loads = [
        (na, sna), (nb, snb), (tk, xk), (lk, slk), (hk, shk), (tv, xv), (lv, slv), (hv, shv),
        (lm, slm), (hm, shm), (tm, xm),
        (lq, slq), (hq, shq), (tq, xq),
    ]
    loads = [pltpu.make_async_copy(s, d, ld.at[i]) for i, (s, d) in enumerate(loads)]
    for c in loads:
        c.start()

    def low_rank(high, low):
        return mix_rate * lax.dot_general(
            high, low, (((0,), (0,)), ((), ())), preferred_element_type=jnp.float32
        )

    def make_narrow(k, base, high, low):
        for j in range(2):
            cols = pl.ds(j * 512, 512)
            b[rows, k, pl.ds(j * 64, 64), :] = (
                base[:, cols].astype(jnp.float32) + low_rank(high[...], low[:, cols])
            ).astype(jnp.bfloat16)

    def copy_to(src, index, send_sem, recv_sem, to):
        return pltpu.make_async_remote_copy(
            src_ref=b.at[src, index], dst_ref=b.at[src, index], send_sem=send_sem,
            recv_sem=recv_sem, device_id=to, device_id_type=MESH,
        )

    def gz_copy(chip, to):
        return pltpu.make_async_remote_copy(
            src_ref=gz.at[chip], dst_ref=gz.at[chip], send_sem=gz_send, recv_sem=gz_recv.at[chip],
            device_id=to, device_id_type=MESH,
        )

    def send_own(k):
        copy_to(rows, k, send.at[0], near_a.at[k], to_up).start()
        copy_to(rows, k, send.at[1], near_b.at[k], to_down).start()

    def to_partner(chip, k):
        copy_to(chip * 2 + core, k, part_send.at[chip], part_recv.at[chip], to_part).start()

    for c in loads[:5]:
        c.wait()
    gain = sna[...] + snb[...]
    gz[z] = jnp.concatenate([gain, gain], axis=1)
    make_narrow(0, xk, shk, slk)
    pl.when(z == 0)(lambda: pl.semaphore_wait(barrier, 8))
    pl.when(z == 2)(lambda: pl.semaphore_wait(barrier, 4))
    pl.when(z % 2 == 1)(lambda: pl.semaphore_wait(barrier, 3))

    @pl.when(z != 0)
    def _():
        gz_copy(z, to_zero).start()

    for c in loads[5:8]:
        c.wait()
    send_own(0)
    make_narrow(1, xv, shv, slv)
    for c in loads[8:]:
        c.wait()
    send_own(1)
    to_partner(z, 0)
    to_partner(z, 1)

    def make_query(i):
        left, top = (i // 4) * 512, (i % 4) * 128
        left, top = pl.multiple_of(left, 512), pl.multiple_of(top, 128)
        part = low_rank(shq[:, pl.ds(top, 128)], slq[:, pl.ds(left, 512)])
        base = xq[pl.ds(left, 512), pl.ds(top, 128)].astype(jnp.float32)
        b[rows, 2 + i] = (base.T + part).astype(jnp.bfloat16)

    def make_mixed(i):
        top = pl.multiple_of(i * 128, 128)
        part = low_rank(shm[:, pl.ds(top, 128)], slm[...])
        base = xm[:, pl.ds(top, 128)].astype(jnp.float32)
        b[rows, 10 + i] = (base.T + part).astype(jnp.bfloat16)

    make_query(0)

    @pl.loop(1, 8)
    def _(i):
        make_query(i)
        send_own(1 + i)
        to_partner(z, 1 + i)

    make_mixed(0)
    send_own(9)
    to_partner(z, 9)

    @pl.loop(1, 8)
    def _(i):
        make_mixed(i)
        send_own(9 + i)
        to_partner(z, 9 + i)

    def tile(ref, src, sems, k, to):
        return pltpu.make_async_remote_copy(
            src_ref=ref.at[src], dst_ref=ref.at[src], send_sem=sems[0].at[k], recv_sem=sems[1].at[k],
            device_id=to, device_id_type=MESH,
        )

    def both(ref, src, sems, one, other):
        return [tile(ref, src, sems, 0, one), tile(ref, src, sems, 1, other)]

    gx_sems, gy_sems, nz_sems = (gx_send, gx_recv), (gy_send, gy_recv), (nz_send, nz_recv)
    gx_near, gx_far = both(gx, x, gx_sems, to_right, to_left), tile(gx, left, gx_sems, 2, to_right)
    gy_near, gy_far = both(gy, y, gy_sems, to_above, to_below), tile(gy, below, gy_sems, 2, to_above)
    nz_part = tile(nz, core, nz_sems, 3, to_part)

    def nz_back(chip):
        return pltpu.make_async_remote_copy(
            src_ref=nz.at[core], dst_ref=nz.at[core], send_sem=nz_send.at[chip - 1], recv_sem=nz_recv.at[0],
            device_id={"rows": chip * 2 + core}, device_id_type=MESH,
        )

    def make_x():
        for i in range(1, 4):
            gz_copy(i, to_up).wait_recv()
        for i in range(4):
            gx[x, i : i + 1] = gz[i]

    def near_x():
        for c in gx_near:
            c.start()

    def far_x():
        for c in gx_near:
            c.wait()
        gx_far.start()

    def make_y():
        gx_far.wait()
        lane = lax.broadcasted_iota(jnp.int32, (4, 128), 1)
        gy[y, 0] = jnp.where(lane < 64, gx[0], gx[1])
        gy[y, 1] = jnp.where(lane < 64, gx[2], gx[3])

    def near_y():
        for c in gy_near:
            c.start()

    def far_y():
        for c in gy_near:
            c.wait()
        gy_far.start()

    def make_z():
        gy_far.wait()
        for i in range(4):
            for k in range(8):
                nz[core, i, k : k + 1] = gy[k // 2, k % 2, i : i + 1]

    def back_z():
        for i in range(1, 4):
            nz_back(i).start()

    gain_steps = [near_x, far_x, make_y, near_y, far_y, make_z, back_z]
    pl.when(z == 0)(make_x)
    send_own(17)
    to_partner(z, 17)

    def pass_on(k, src):
        way, sem, to = ((2, far_a, to_up), (3, far_b, to_down))[k % 2]
        return copy_to(src, k, send.at[way], sem.at[k // 2], to)

    def pass_late(way, n, src):
        (piece, first, count), to = ((WAY_UP, WAY_DOWN)[way][n], (to_up, to_down)[way])
        some = pl.ds(first, count)
        return pltpu.make_async_remote_copy(
            src_ref=b.at[src, piece, some], dst_ref=late.at[piece, some], send_sem=late_send.at[way, n],
            recv_sem=late_recv.at[way, n], device_id=to, device_id_type=MESH,
        )

    below_chip, above_chip = down * 2 + core, up * 2 + core
    far_chip = far * 2 + core
    for k in range(PIECES):
        copy_to(below_chip, k, send.at[0], near_a.at[k], to_up).wait_recv()
        if k >= 2 and k % 2 == 0:
            pass_on(k, below_chip).start()
        to_partner(down, k)
        copy_to(above_chip, k, send.at[1], near_b.at[k], to_down).wait_recv()
        if k >= 2 and k % 2 == 1:
            pass_on(k, above_chip).start()
        to_partner(up, k)
        if k < len(gain_steps):
            pl.when(z == 0)(gain_steps[k])

    late_copies = [pass_late(0, n, below_chip) for n in range(len(WAY_UP))]
    late_copies += [pass_late(1, n, above_chip) for n in range(len(WAY_DOWN))]
    for c in late_copies:
        c.start()

    def far_pieces(first, last):
        @pl.loop(first, last)
        def _(j):
            copy_to(far_chip, 2 * j, send.at[2], far_a.at[j], to_up).wait_recv()
            to_partner(far, 2 * j)
            copy_to(far_chip, 2 * j + 1, send.at[3], far_b.at[j], to_down).wait_recv()
            to_partner(far, 2 * j + 1)

    far_pieces(1, 6)

    @pl.when(z != 0)
    def _():
        gz_copy(z, to_zero).wait_send()
        nz_back(1).wait_recv()

    @pl.when(z == 0)
    def _():
        for i in range(1, 4):
            nz_back(i).wait_send()

    nz_part.start()
    far_pieces(6, 9)
    nz_part.wait()

    def all_of(src, count, send_sem, recv_sem, to):
        part = b.at[src, pl.ds(0, count)]
        return pltpu.make_async_remote_copy(
            src_ref=part, dst_ref=part, send_sem=send_sem, recv_sem=recv_sem,
            device_id=to, device_id_type=MESH,
        )

    all_of(rows, PIECES, send.at[0], near_a.at[0], to_up).wait_send()
    all_of(rows, PIECES, send.at[1], near_b.at[0], to_down).wait_send()
    all_of(rows, 8, send.at[2], far_a.at[0], to_up).wait_send()
    all_of(rows, 8, send.at[3], far_b.at[0], to_down).wait_send()
    for chip, count in ((z, PIECES), (up, PIECES), (down, PIECES), (far, PIECES - 2)):
        all_of(chip * 2 + core, count, part_send.at[chip], part_recv.at[chip], to_part).wait_send()
        all_of(chip * 2 + 1 - core, count, part_send.at[chip], part_recv.at[chip], to_part).wait_recv()
    for c in late_copies:
        c.wait()


def comm(*args):
    bf16, f32 = jnp.bfloat16, jnp.float32
    dma = pltpu.SemaphoreType.DMA
    return pl.pallas_call(
        comm_kernel,
        out_shape=[
            pltpu.VMEM((8, PIECES, 128, 512), bf16), pltpu.VMEM((2, 128, 512), bf16), pltpu.VMEM((2, 4, 8, 128), f32),
        ],
        in_specs=[HBM] * len(args),
        out_specs=[VMEM] * 3,
        scratch_shapes=[
            pltpu.VMEM((1024, 512), bf16), pltpu.VMEM((64, 1024), bf16), pltpu.VMEM((64, 1024), bf16),
            pltpu.VMEM((512, 1024), bf16),
            pltpu.VMEM((16, 1024), bf16), pltpu.VMEM((16, 512), bf16),
            pltpu.VMEM((16, 1024), bf16), pltpu.VMEM((16, 64), bf16),
            pltpu.VMEM((16, 1024), bf16), pltpu.VMEM((16, 64), bf16),
            pltpu.VMEM((16, 512), bf16), pltpu.VMEM((16, 1024), bf16),
            pltpu.VMEM((1, 64), f32), pltpu.VMEM((1, 64), f32),
            pltpu.VMEM((4, 1, 128), f32), pltpu.VMEM((4, 4, 128), f32), pltpu.VMEM((4, 2, 4, 128), f32),
            dma((14,)), dma((4,)), dma((PIECES,)), dma((PIECES,)), dma((PIECES // 2,)), dma((PIECES // 2,)),
            dma((4,)), dma((4,)),
            dma, dma((4,)), dma((3,)), dma((3,)), dma((3,)), dma((3,)), dma((4,)), dma((4,)),
            dma((2, 2)), dma((2, 2)),
        ],
        compiler_params=pltpu.CompilerParams(
            collective_id=0, has_side_effects=True, vmem_limit_bytes=44 * 2**20
        ),
        name="comm",
    )(*args)


def put_narrow(r, block, k, v, sem):
    for i, out in enumerate((k, v)):
        for j in range(2):
            cols = pl.ds(pl.multiple_of(r * 1024 + j * 512, 512), 512)
            pltpu.make_async_copy(block.at[i, pl.ds(j * 64, 64)], out.at[:, cols], sem.at[i]).start()


def write_kernel(b, late, nz, q, k, v, m, n, gain, sem):
    tiles = [nz[r % 2, r // 2] for r in range(8)]
    gain[...] = jnp.concatenate(tiles, axis=0).astype(jnp.bfloat16)
    for r in range(8):
        pltpu.make_async_copy(b.at[r, pl.ds(10, 8)], m.at[pl.ds(r * 8, 8)], sem.at[3]).start()
        for j in range(2):
            cols = pl.ds(r * 1024 + j * 512, 512)
            pltpu.make_async_copy(b.at[r, pl.ds(2 + 4 * j, 4)], q.at[:, :, cols], sem.at[2]).start()
    rows = lax.axis_index("rows")
    core = rows % 2
    far = (rows // 2 + 2) % 4 * 2
    for d in range(2, 8):
        r = (far + d) % 8
        put_narrow(r, b.at[r, pl.ds(0, 2)], k, v, sem)
    put_narrow(far + core, late, k, v, sem)
    pltpu.make_async_copy(gain, n, sem.at[4]).start()
    for i, ref in enumerate((k.at[:, pl.ds(0, 7168)], v.at[:, pl.ds(0, 7168)], q, m, n)):
        pltpu.make_async_copy(ref, ref, sem.at[i]).wait()


def write(b, late, nz):
    bf16 = jnp.bfloat16
    shapes = [(4, 128, 8192), (64, 8192), (64, 8192), (64, 128, 512), (64, 128)]
    return pl.pallas_call(
        write_kernel,
        out_shape=[jax.ShapeDtypeStruct(s, bf16) for s in shapes],
        in_specs=[VMEM] * 3,
        out_specs=[HBM] * 5,
        scratch_shapes=[pltpu.VMEM((64, 128), bf16), pltpu.SemaphoreType.DMA((5,))],
        compiler_params=pltpu.CompilerParams(vmem_limit_bytes=4 * 2**20),
        cost_estimate=pl.CostEstimate(flops=0, bytes_accessed=38 * 2**20, transcendentals=0),
        name="write",
    )(b, late, nz)


def last_kernel(other, k_in, v_in, k, v, sem):
    rows = lax.axis_index("rows")
    put_narrow((rows // 2 + 2) % 4 * 2 + 1 - rows % 2, other, k, v, sem)
    for i, ref in enumerate((k, v)):
        part = ref.at[:, pl.ds(0, 1024)]
        pltpu.make_async_copy(part, part, sem.at[i]).wait()


def write_last(other, k, v):
    return pl.pallas_call(
        last_kernel,
        out_shape=[jax.ShapeDtypeStruct(a.shape, a.dtype) for a in (k, v)],
        in_specs=[VMEM, HBM, HBM],
        out_specs=[HBM] * 2,
        scratch_shapes=[pltpu.SemaphoreType.DMA((2,))],
        input_output_aliases={1: 0, 2: 1},
        compiler_params=pltpu.CompilerParams(vmem_limit_bytes=2**20),
        name="write_last",
    )(other, k, v)


def body(
    train_query, low_query, high_query, train_key, low_key, high_key, train_value, low_value, high_value,
    train_mixed, low_mixed, high_mixed, norm_train, norm_step,
):
    b, late, nz = comm(
        train_query, train_key.T, train_value.T, train_mixed,
        low_query.T, high_query, low_key.T, high_key, low_value.T, high_value, low_mixed.T, high_mixed,
        norm_train.reshape(1, 64), norm_step.reshape(1, 64),
    )
    other = lax.ppermute(late, "rows", [(r, r + 1 - 2 * (r % 2)) for r in range(8)])
    q, k, v, m, n = write(b, late, nz)
    k, v = write_last(other, k, v)
    return q.reshape(512, 8192), k, v, m.reshape(8192, 512), n.reshape(8192)


def solution(mesh):
    R, M = "rows", "model"
    return jax.shard_map(
        body,
        mesh=mesh,
        in_specs=(
            P(R, M), P(R, None), P(None, M),
            P(R, M), P(R, None), P(None, M),
            P(R, M), P(R, None), P(None, M),
            P(M, R), P(M, None), P(None, R),
            P((R, M)), P((R, M)),
        ),
        out_specs=(P(M, None), P(M, None), P(M, None), P(None, M), P()),
        check_vma=False,
    )
```

```python
import jax
import jax.numpy as jnp
from jax import lax
from jax.experimental import pallas as pl
from jax.experimental.pallas import tpu as pltpu
from jax.sharding import PartitionSpec as P

MESH = pl.DeviceIdType.MESH
HBM = pl.BlockSpec(memory_space=pltpu.HBM)
VMEM = pl.BlockSpec(memory_space=pltpu.VMEM)

mix_rate = 0.5

PIECES = 18

SPLIT = 96
WAY_UP = ((0, 0, SPLIT),)
WAY_DOWN = ((0, SPLIT, 128 - SPLIT), (1, 0, 128)) if SPLIT < 128 else ((1, 0, 128),)


def comm_kernel(
    tq, tk, tv, tm, lq, hq, lk, hk, lv, hv, lm, hm, na, nb,
    b, late, nz,
    xq, xk, xv, xm, slq, shq, slk, shk, slv, shv, slm, shm, sna, snb, gz, gx, gy,
    ld, send, near_a, near_b, far_a, far_b, part_send, part_recv,
    gz_send, gz_recv, gx_send, gx_recv, gy_send, gy_recv, nz_send, nz_recv,
    late_send, late_recv, early_send, early_recv,
):
    rows = lax.axis_index("rows")
    model = lax.axis_index("model")
    z, core = rows // 2, rows % 2
    y, x = model // 4, model % 4
    up, down = (z + 1) % 4, (z + 3) % 4
    far = (z + 2) % 4
    right, left, above, below = (x + 1) % 4, (x + 3) % 4, (y + 1) % 4, (y + 3) % 4
    to_up = {"rows": up * 2 + core}
    to_down = {"rows": down * 2 + core}
    to_part = {"rows": z * 2 + 1 - core}
    to_far, to_zero = {"rows": far * 2 + core}, {"rows": core}
    to_right, to_left = {"model": y * 4 + right}, {"model": y * 4 + left}
    to_above, to_below = {"model": above * 4 + x}, {"model": below * 4 + x}

    barrier = pltpu.get_barrier_semaphore()
    for peer in (to_up, to_down, to_part):
        pl.semaphore_signal(barrier, inc=1, device_id=peer, device_id_type=MESH)

    @pl.when(z == 0)
    def _():
        for peer in (to_far, to_right, to_left, to_above, to_below):
            pl.semaphore_signal(barrier, inc=1, device_id=peer, device_id_type=MESH)

    @pl.when(z == 2)
    def _():
        pl.semaphore_signal(barrier, inc=1, device_id=to_far, device_id_type=MESH)

    loads = [
        (na, sna), (nb, snb), (tk, xk), (lk, slk), (hk, shk), (tv, xv), (lv, slv), (hv, shv),
        (lm, slm), (hm, shm), (tm, xm),
        (lq, slq), (hq, shq), (tq, xq),
    ]
    loads = [pltpu.make_async_copy(s, d, ld.at[i]) for i, (s, d) in enumerate(loads)]
    for c in loads:
        c.start()

    def low_rank(high, low):
        return mix_rate * lax.dot_general(
            high, low, (((0,), (0,)), ((), ())), preferred_element_type=jnp.float32
        )

    def make_narrow(k, base, high, low):
        for j in range(2):
            cols = pl.ds(j * 512, 512)
            b[rows, k, pl.ds(j * 64, 64), :] = (
                base[:, cols].astype(jnp.float32) + low_rank(high[...], low[:, cols])
            ).astype(jnp.bfloat16)

    def copy_to(src, index, send_sem, recv_sem, to):
        return pltpu.make_async_remote_copy(
            src_ref=b.at[src, index], dst_ref=b.at[src, index], send_sem=send_sem,
            recv_sem=recv_sem, device_id=to, device_id_type=MESH,
        )

    def gz_copy(chip, to):
        return pltpu.make_async_remote_copy(
            src_ref=gz.at[chip], dst_ref=gz.at[chip], send_sem=gz_send, recv_sem=gz_recv.at[chip],
            device_id=to, device_id_type=MESH,
        )

    def send_own(k):
        copy_to(rows, k, send.at[0], near_a.at[k], to_up).start()
        copy_to(rows, k, send.at[1], near_b.at[k], to_down).start()

    def to_partner(chip, k):
        copy_to(chip * 2 + core, k, part_send.at[chip], part_recv.at[chip], to_part).start()

    def early(chip, k):
        return copy_to(chip * 2 + core, k, early_send.at[chip, k], early_recv.at[chip, k], to_part)

    for c in loads[:5]:
        c.wait()
    gain = sna[...] + snb[...]
    gz[z] = jnp.concatenate([gain, gain], axis=1)
    make_narrow(0, xk, shk, slk)
    pl.when(z == 0)(lambda: pl.semaphore_wait(barrier, 8))
    pl.when(z == 2)(lambda: pl.semaphore_wait(barrier, 4))
    pl.when(z % 2 == 1)(lambda: pl.semaphore_wait(barrier, 3))

    @pl.when(z != 0)
    def _():
        gz_copy(z, to_zero).start()

    for c in loads[5:8]:
        c.wait()
    send_own(0)
    make_narrow(1, xv, shv, slv)
    for c in loads[8:]:
        c.wait()
    send_own(1)
    to_partner(z, 0)
    to_partner(z, 1)

    def make_query(i):
        left, top = (i // 4) * 512, (i % 4) * 128
        left, top = pl.multiple_of(left, 512), pl.multiple_of(top, 128)
        part = low_rank(shq[:, pl.ds(top, 128)], slq[:, pl.ds(left, 512)])
        base = xq[pl.ds(left, 512), pl.ds(top, 128)].astype(jnp.float32)
        b[rows, 2 + i] = (base.T + part).astype(jnp.bfloat16)

    def make_mixed(i):
        top = pl.multiple_of(i * 128, 128)
        part = low_rank(shm[:, pl.ds(top, 128)], slm[...])
        base = xm[:, pl.ds(top, 128)].astype(jnp.float32)
        b[rows, 10 + i] = (base.T + part).astype(jnp.bfloat16)

    make_query(0)

    @pl.loop(1, 8)
    def _(i):
        make_query(i)
        send_own(1 + i)
        to_partner(z, 1 + i)

    make_mixed(0)
    send_own(9)
    to_partner(z, 9)

    @pl.loop(1, 8)
    def _(i):
        make_mixed(i)
        send_own(9 + i)
        to_partner(z, 9 + i)

    def tile(ref, src, sems, k, to):
        return pltpu.make_async_remote_copy(
            src_ref=ref.at[src], dst_ref=ref.at[src], send_sem=sems[0].at[k], recv_sem=sems[1].at[k],
            device_id=to, device_id_type=MESH,
        )

    def both(ref, src, sems, one, other):
        return [tile(ref, src, sems, 0, one), tile(ref, src, sems, 1, other)]

    gx_sems, gy_sems, nz_sems = (gx_send, gx_recv), (gy_send, gy_recv), (nz_send, nz_recv)
    gx_near, gx_far = both(gx, x, gx_sems, to_right, to_left), tile(gx, left, gx_sems, 2, to_right)
    gy_near, gy_far = both(gy, y, gy_sems, to_above, to_below), tile(gy, below, gy_sems, 2, to_above)
    nz_part = tile(nz, core, nz_sems, 3, to_part)

    def nz_back(chip):
        return pltpu.make_async_remote_copy(
            src_ref=nz.at[core], dst_ref=nz.at[core], send_sem=nz_send.at[chip - 1], recv_sem=nz_recv.at[0],
            device_id={"rows": chip * 2 + core}, device_id_type=MESH,
        )

    def make_x():
        for i in range(1, 4):
            gz_copy(i, to_up).wait_recv()
        for i in range(4):
            gx[x, i : i + 1] = gz[i]

    def near_x():
        for c in gx_near:
            c.start()

    def far_x():
        for c in gx_near:
            c.wait()
        gx_far.start()

    def make_y():
        gx_far.wait()
        lane = lax.broadcasted_iota(jnp.int32, (4, 128), 1)
        gy[y, 0] = jnp.where(lane < 64, gx[0], gx[1])
        gy[y, 1] = jnp.where(lane < 64, gx[2], gx[3])

    def near_y():
        for c in gy_near:
            c.start()

    def far_y():
        for c in gy_near:
            c.wait()
        gy_far.start()

    def make_z():
        gy_far.wait()
        for i in range(4):
            for k in range(8):
                nz[core, i, k : k + 1] = gy[k // 2, k % 2, i : i + 1]

    def back_z():
        for i in range(1, 4):
            nz_back(i).start()

    gain_steps = [near_x, far_x, make_y, near_y, far_y, make_z, back_z]
    pl.when(z == 0)(make_x)
    send_own(17)
    to_partner(z, 17)

    def pass_on(k, src):
        way, sem, to = ((2, far_a, to_up), (3, far_b, to_down))[k % 2]
        return copy_to(src, k, send.at[way], sem.at[k // 2], to)

    def pass_late(way, n, of):
        (piece, first, count), to = ((WAY_UP, WAY_DOWN)[way][n], (to_up, to_down)[way])
        some = pl.ds(first, count)
        return pltpu.make_async_remote_copy(
            src_ref=b.at[(down, up)[way] * 2 + of, piece, some], dst_ref=late.at[of, piece, some],
            send_sem=late_send.at[of, way, n], recv_sem=late_recv.at[of, way, n], device_id=to, device_id_type=MESH,
        )

    below_chip, above_chip = down * 2 + core, up * 2 + core
    far_chip = far * 2 + core
    for k in range(PIECES):
        copy_to(below_chip, k, send.at[0], near_a.at[k], to_up).wait_recv()
        if k >= 2 and k % 2 == 0:
            pass_on(k, below_chip).start()
        early(down, k).start() if k < 2 else to_partner(down, k)
        copy_to(above_chip, k, send.at[1], near_b.at[k], to_down).wait_recv()
        if k >= 2 and k % 2 == 1:
            pass_on(k, above_chip).start()
        early(up, k).start() if k < 2 else to_partner(up, k)
        if k < len(gain_steps):
            pl.when(z == 0)(gain_steps[k])

    for chip in (down, up):
        for k in range(2):
            early(chip, k).wait()
    late_parts = [(0, n, of) for n in range(len(WAY_UP)) for of in range(2)]
    late_parts += [(1, n, of) for n in range(len(WAY_DOWN)) for of in range(2)]

    @pl.when(core == 1)
    def _():
        for part in late_parts:
            pass_late(*part).start()

    def far_pieces(first, last):
        @pl.loop(first, last)
        def _(j):
            copy_to(far_chip, 2 * j, send.at[2], far_a.at[j], to_up).wait_recv()
            to_partner(far, 2 * j)
            copy_to(far_chip, 2 * j + 1, send.at[3], far_b.at[j], to_down).wait_recv()
            to_partner(far, 2 * j + 1)

    far_pieces(1, 6)

    @pl.when(z != 0)
    def _():
        gz_copy(z, to_zero).wait_send()
        nz_back(1).wait_recv()

    @pl.when(z == 0)
    def _():
        for i in range(1, 4):
            nz_back(i).wait_send()

    nz_part.start()
    far_pieces(6, 9)
    nz_part.wait()

    def all_of(src, count, send_sem, recv_sem, to):
        part = b.at[src, pl.ds(0, count)]
        return pltpu.make_async_remote_copy(
            src_ref=part, dst_ref=part, send_sem=send_sem, recv_sem=recv_sem,
            device_id=to, device_id_type=MESH,
        )

    all_of(rows, PIECES, send.at[0], near_a.at[0], to_up).wait_send()
    all_of(rows, PIECES, send.at[1], near_b.at[0], to_down).wait_send()
    all_of(rows, 8, send.at[2], far_a.at[0], to_up).wait_send()
    all_of(rows, 8, send.at[3], far_b.at[0], to_down).wait_send()
    for chip, count in ((z, PIECES), (up, PIECES - 2), (down, PIECES - 2), (far, PIECES - 2)):
        all_of(chip * 2 + core, count, part_send.at[chip], part_recv.at[chip], to_part).wait_send()
        all_of(chip * 2 + 1 - core, count, part_send.at[chip], part_recv.at[chip], to_part).wait_recv()

    @pl.when(core == 1)
    def _():
        for part in late_parts:
            pass_late(*part).wait()


def comm(*args):
    bf16, f32 = jnp.bfloat16, jnp.float32
    dma = pltpu.SemaphoreType.DMA
    return pl.pallas_call(
        comm_kernel,
        out_shape=[
            pltpu.VMEM((8, PIECES, 128, 512), bf16), pltpu.VMEM((2, 2, 128, 512), bf16),
            pltpu.VMEM((2, 4, 8, 128), f32),
        ],
        in_specs=[HBM] * len(args),
        out_specs=[VMEM] * 3,
        scratch_shapes=[
            pltpu.VMEM((1024, 512), bf16), pltpu.VMEM((64, 1024), bf16), pltpu.VMEM((64, 1024), bf16),
            pltpu.VMEM((512, 1024), bf16),
            pltpu.VMEM((16, 1024), bf16), pltpu.VMEM((16, 512), bf16),
            pltpu.VMEM((16, 1024), bf16), pltpu.VMEM((16, 64), bf16),
            pltpu.VMEM((16, 1024), bf16), pltpu.VMEM((16, 64), bf16),
            pltpu.VMEM((16, 512), bf16), pltpu.VMEM((16, 1024), bf16),
            pltpu.VMEM((1, 64), f32), pltpu.VMEM((1, 64), f32),
            pltpu.VMEM((4, 1, 128), f32), pltpu.VMEM((4, 4, 128), f32), pltpu.VMEM((4, 2, 4, 128), f32),
            dma((14,)), dma((4,)), dma((PIECES,)), dma((PIECES,)), dma((PIECES // 2,)), dma((PIECES // 2,)),
            dma((4,)), dma((4,)),
            dma, dma((4,)), dma((3,)), dma((3,)), dma((3,)), dma((3,)), dma((4,)), dma((4,)),
            dma((2, 2, 2)), dma((2, 2, 2)), dma((4, 2)), dma((4, 2)),
        ],
        compiler_params=pltpu.CompilerParams(
            collective_id=0, has_side_effects=True, vmem_limit_bytes=44 * 2**20
        ),
        name="comm",
    )(*args)


def put_narrow(r, block, k, v, sem):
    for i, out in enumerate((k, v)):
        for j in range(2):
            cols = pl.ds(pl.multiple_of(r * 1024 + j * 512, 512), 512)
            pltpu.make_async_copy(block.at[i, pl.ds(j * 64, 64)], out.at[:, cols], sem.at[i]).start()


def write_kernel(b, late, nz, q, k, v, m, n, gain, sem):
    tiles = [nz[r % 2, r // 2] for r in range(8)]
    gain[...] = jnp.concatenate(tiles, axis=0).astype(jnp.bfloat16)
    for r in range(8):
        pltpu.make_async_copy(b.at[r, pl.ds(10, 8)], m.at[pl.ds(r * 8, 8)], sem.at[3]).start()
        for j in range(2):
            cols = pl.ds(r * 1024 + j * 512, 512)
            pltpu.make_async_copy(b.at[r, pl.ds(2 + 4 * j, 4)], q.at[:, :, cols], sem.at[2]).start()
    rows = lax.axis_index("rows")
    core = rows % 2
    far = (rows // 2 + 2) % 4 * 2
    for d in range(2, 8):
        r = (far + d) % 8
        put_narrow(r, b.at[r, pl.ds(0, 2)], k, v, sem)
    pltpu.make_async_copy(gain, n, sem.at[4]).start()

    def wait(i, ref):
        pltpu.make_async_copy(ref, ref, sem.at[i]).wait()

    @pl.when(core == 1)
    def _():
        for of in range(2):
            put_narrow(far + of, late.at[of], k, v, sem)
        wait(0, k)
        wait(1, v)

    @pl.when(core == 0)
    def _():
        wait(0, k.at[:, pl.ds(0, 6144)])
        wait(1, v.at[:, pl.ds(0, 6144)])

    for i, ref in ((2, q), (3, m), (4, n)):
        wait(i, ref)


def write(b, late, nz):
    bf16 = jnp.bfloat16
    shapes = [(4, 128, 8192), (64, 8192), (64, 8192), (64, 128, 512), (64, 128)]
    return pl.pallas_call(
        write_kernel,
        out_shape=[jax.ShapeDtypeStruct(s, bf16) for s in shapes],
        in_specs=[VMEM] * 3,
        out_specs=[HBM] * 5,
        scratch_shapes=[pltpu.VMEM((64, 128), bf16), pltpu.SemaphoreType.DMA((5,))],
        compiler_params=pltpu.CompilerParams(vmem_limit_bytes=4 * 2**20),
        cost_estimate=pl.CostEstimate(flops=0, bytes_accessed=38 * 2**20, transcendentals=0),
        name="write",
    )(b, late, nz)


def last_kernel(other, k_in, v_in, k, v, sem):
    rows = lax.axis_index("rows")
    far = (rows // 2 + 2) % 4 * 2

    @pl.when(rows % 2 == 0)
    def _():
        for of in range(2):
            put_narrow(far + of, other.at[of], k, v, sem)
        for i, ref in enumerate((k, v)):
            part = ref.at[:, pl.ds(0, 2048)]
            pltpu.make_async_copy(part, part, sem.at[i]).wait()


def write_last(other, k, v):
    return pl.pallas_call(
        last_kernel,
        out_shape=[jax.ShapeDtypeStruct(a.shape, a.dtype) for a in (k, v)],
        in_specs=[VMEM, HBM, HBM],
        out_specs=[HBM] * 2,
        scratch_shapes=[pltpu.SemaphoreType.DMA((2,))],
        input_output_aliases={1: 0, 2: 1},
        compiler_params=pltpu.CompilerParams(vmem_limit_bytes=2**20),
        name="write_last",
    )(other, k, v)


def body(
    train_query, low_query, high_query, train_key, low_key, high_key, train_value, low_value, high_value,
    train_mixed, low_mixed, high_mixed, norm_train, norm_step,
):
    b, late, nz = comm(
        train_query, train_key.T, train_value.T, train_mixed,
        low_query.T, high_query, low_key.T, high_key, low_value.T, high_value, low_mixed.T, high_mixed,
        norm_train.reshape(1, 64), norm_step.reshape(1, 64),
    )
    other = lax.ppermute(late, "rows", [(r, r + 1 - 2 * (r % 2)) for r in range(8)])
    q, k, v, m, n = write(b, late, nz)
    k, v = write_last(other, k, v)
    return q.reshape(512, 8192), k, v, m.reshape(8192, 512), n.reshape(8192)


def solution(mesh):
    R, M = "rows", "model"
    return jax.shard_map(
        body,
        mesh=mesh,
        in_specs=(
            P(R, M), P(R, None), P(None, M),
            P(R, M), P(R, None), P(None, M),
            P(R, M), P(R, None), P(None, M),
            P(M, R), P(M, None), P(None, R),
            P((R, M)), P((R, M)),
        ),
        out_specs=(P(M, None), P(M, None), P(M, None), P(None, M), P()),
        check_vma=False,
    )
```

```python
import jax
import jax.numpy as jnp
from jax import lax
from jax.experimental import pallas as pl
from jax.experimental.pallas import tpu as pltpu
from jax.sharding import PartitionSpec as P

MESH = pl.DeviceIdType.MESH
HBM = pl.BlockSpec(memory_space=pltpu.HBM)
VMEM = pl.BlockSpec(memory_space=pltpu.VMEM)

mix_rate = 0.5

PIECES = 18

SPLIT = 112
WAY_UP = ((0, 0, SPLIT),)
WAY_DOWN = ((0, SPLIT, 128 - SPLIT), (1, 0, 128)) if SPLIT < 128 else ((1, 0, 128),)


def comm_kernel(
    tq, tk, tv, tm, lq, hq, lk, hk, lv, hv, lm, hm, na, nb,
    b, late, nz,
    xq, xk, xv, xm, slq, shq, slk, shk, slv, shv, slm, shm, sna, snb, gz, gx, gy,
    ld, send, near_a, near_b, far_a, far_b, part_send, part_recv,
    gz_send, gz_recv, gx_send, gx_recv, gy_send, gy_recv, nz_send, nz_recv,
    late_send, late_recv, early_send, early_recv,
):
    rows = lax.axis_index("rows")
    model = lax.axis_index("model")
    z, core = rows // 2, rows % 2
    y, x = model // 4, model % 4
    up, down = (z + 1) % 4, (z + 3) % 4
    far = (z + 2) % 4
    right, left, above, below = (x + 1) % 4, (x + 3) % 4, (y + 1) % 4, (y + 3) % 4
    to_up = {"rows": up * 2 + core}
    to_down = {"rows": down * 2 + core}
    to_part = {"rows": z * 2 + 1 - core}
    to_far, to_zero = {"rows": far * 2 + core}, {"rows": core}
    to_right, to_left = {"model": y * 4 + right}, {"model": y * 4 + left}
    to_above, to_below = {"model": above * 4 + x}, {"model": below * 4 + x}

    barrier = pltpu.get_barrier_semaphore()
    for peer in (to_up, to_down, to_part):
        pl.semaphore_signal(barrier, inc=1, device_id=peer, device_id_type=MESH)

    @pl.when(z == 0)
    def _():
        for peer in (to_far, to_right, to_left, to_above, to_below):
            pl.semaphore_signal(barrier, inc=1, device_id=peer, device_id_type=MESH)

    @pl.when(z == 2)
    def _():
        pl.semaphore_signal(barrier, inc=1, device_id=to_far, device_id_type=MESH)

    loads = [
        (na, sna), (nb, snb), (tk, xk), (lk, slk), (hk, shk), (tv, xv), (lv, slv), (hv, shv),
        (lm, slm), (hm, shm), (tm, xm),
        (lq, slq), (hq, shq), (tq, xq),
    ]
    loads = [pltpu.make_async_copy(s, d, ld.at[i]) for i, (s, d) in enumerate(loads)]
    for c in loads:
        c.start()

    def low_rank(high, low):
        return mix_rate * lax.dot_general(
            high, low, (((0,), (0,)), ((), ())), preferred_element_type=jnp.float32
        )

    def make_narrow(k, base, high, low):
        for j in range(2):
            cols = pl.ds(j * 512, 512)
            b[rows, k, pl.ds(j * 64, 64), :] = (
                base[:, cols].astype(jnp.float32) + low_rank(high[...], low[:, cols])
            ).astype(jnp.bfloat16)

    def copy_to(src, index, send_sem, recv_sem, to):
        return pltpu.make_async_remote_copy(
            src_ref=b.at[src, index], dst_ref=b.at[src, index], send_sem=send_sem,
            recv_sem=recv_sem, device_id=to, device_id_type=MESH,
        )

    def gz_copy(chip, to):
        return pltpu.make_async_remote_copy(
            src_ref=gz.at[chip], dst_ref=gz.at[chip], send_sem=gz_send, recv_sem=gz_recv.at[chip],
            device_id=to, device_id_type=MESH,
        )

    def send_own(k):
        copy_to(rows, k, send.at[0], near_a.at[k], to_up).start()
        copy_to(rows, k, send.at[1], near_b.at[k], to_down).start()

    def to_partner(chip, k):
        copy_to(chip * 2 + core, k, part_send.at[chip], part_recv.at[chip], to_part).start()

    def early(chip, k):
        return copy_to(chip * 2 + core, k, early_send.at[chip, k], early_recv.at[chip, k], to_part)

    for c in loads[:5]:
        c.wait()
    gain = sna[...] + snb[...]
    gz[z] = jnp.concatenate([gain, gain], axis=1)
    make_narrow(0, xk, shk, slk)
    pl.when(z == 0)(lambda: pl.semaphore_wait(barrier, 8))
    pl.when(z == 2)(lambda: pl.semaphore_wait(barrier, 4))
    pl.when(z % 2 == 1)(lambda: pl.semaphore_wait(barrier, 3))

    @pl.when(z != 0)
    def _():
        gz_copy(z, to_zero).start()

    for c in loads[5:8]:
        c.wait()
    send_own(0)
    make_narrow(1, xv, shv, slv)
    for c in loads[8:]:
        c.wait()
    send_own(1)
    to_partner(z, 0)
    to_partner(z, 1)

    def make_query(i):
        left, top = (i // 4) * 512, (i % 4) * 128
        left, top = pl.multiple_of(left, 512), pl.multiple_of(top, 128)
        part = low_rank(shq[:, pl.ds(top, 128)], slq[:, pl.ds(left, 512)])
        base = xq[pl.ds(left, 512), pl.ds(top, 128)].astype(jnp.float32)
        b[rows, 2 + i] = (base.T + part).astype(jnp.bfloat16)

    def make_mixed(i):
        top = pl.multiple_of(i * 128, 128)
        part = low_rank(shm[:, pl.ds(top, 128)], slm[...])
        base = xm[:, pl.ds(top, 128)].astype(jnp.float32)
        b[rows, 10 + i] = (base.T + part).astype(jnp.bfloat16)

    make_query(0)

    @pl.loop(1, 8)
    def _(i):
        make_query(i)
        send_own(1 + i)
        to_partner(z, 1 + i)

    make_mixed(0)
    send_own(9)
    to_partner(z, 9)

    @pl.loop(1, 8)
    def _(i):
        make_mixed(i)
        send_own(9 + i)
        to_partner(z, 9 + i)

    def tile(ref, src, sems, k, to):
        return pltpu.make_async_remote_copy(
            src_ref=ref.at[src], dst_ref=ref.at[src], send_sem=sems[0].at[k], recv_sem=sems[1].at[k],
            device_id=to, device_id_type=MESH,
        )

    def both(ref, src, sems, one, other):
        return [tile(ref, src, sems, 0, one), tile(ref, src, sems, 1, other)]

    gx_sems, gy_sems, nz_sems = (gx_send, gx_recv), (gy_send, gy_recv), (nz_send, nz_recv)
    gx_near, gx_far = both(gx, x, gx_sems, to_right, to_left), tile(gx, left, gx_sems, 2, to_right)
    gy_near, gy_far = both(gy, y, gy_sems, to_above, to_below), tile(gy, below, gy_sems, 2, to_above)
    nz_part = tile(nz, core, nz_sems, 3, to_part)

    def nz_back(chip):
        return pltpu.make_async_remote_copy(
            src_ref=nz.at[core], dst_ref=nz.at[core], send_sem=nz_send.at[chip - 1], recv_sem=nz_recv.at[0],
            device_id={"rows": chip * 2 + core}, device_id_type=MESH,
        )

    def make_x():
        for i in range(1, 4):
            gz_copy(i, to_up).wait_recv()
        for i in range(4):
            gx[x, i : i + 1] = gz[i]

    def near_x():
        for c in gx_near:
            c.start()

    def far_x():
        for c in gx_near:
            c.wait()
        gx_far.start()

    def make_y():
        gx_far.wait()
        lane = lax.broadcasted_iota(jnp.int32, (4, 128), 1)
        gy[y, 0] = jnp.where(lane < 64, gx[0], gx[1])
        gy[y, 1] = jnp.where(lane < 64, gx[2], gx[3])

    def near_y():
        for c in gy_near:
            c.start()

    def far_y():
        for c in gy_near:
            c.wait()
        gy_far.start()

    def make_z():
        gy_far.wait()
        for i in range(4):
            for k in range(8):
                nz[core, i, k : k + 1] = gy[k // 2, k % 2, i : i + 1]

    def back_z():
        for i in range(1, 4):
            nz_back(i).start()

    gain_steps = [near_x, far_x, make_y, near_y, far_y, make_z, back_z]
    pl.when(z == 0)(make_x)
    send_own(17)
    to_partner(z, 17)

    def pass_on(k, src):
        way, sem, to = ((2, far_a, to_up), (3, far_b, to_down))[k % 2]
        return copy_to(src, k, send.at[way], sem.at[k // 2], to)

    def pass_late(way, n, of):
        (piece, first, count), to = ((WAY_UP, WAY_DOWN)[way][n], (to_up, to_down)[way])
        some = pl.ds(first, count)
        return pltpu.make_async_remote_copy(
            src_ref=b.at[(down, up)[way] * 2 + of, piece, some], dst_ref=late.at[of, piece, some],
            send_sem=late_send.at[of, way, n], recv_sem=late_recv.at[of, way, n], device_id=to, device_id_type=MESH,
        )

    below_chip, above_chip = down * 2 + core, up * 2 + core
    far_chip = far * 2 + core
    for k in range(PIECES):
        copy_to(below_chip, k, send.at[0], near_a.at[k], to_up).wait_recv()
        if k >= 2 and k % 2 == 0:
            pass_on(k, below_chip).start()
        early(down, k).start() if k < 2 else to_partner(down, k)
        copy_to(above_chip, k, send.at[1], near_b.at[k], to_down).wait_recv()
        if k >= 2 and k % 2 == 1:
            pass_on(k, above_chip).start()
        early(up, k).start() if k < 2 else to_partner(up, k)
        if k < len(gain_steps):
            pl.when(z == 0)(gain_steps[k])

    for chip in (down, up):
        for k in range(2):
            early(chip, k).wait()
    late_parts = [(0, n, of) for n in range(len(WAY_UP)) for of in range(2)]
    late_parts += [(1, n, of) for n in range(len(WAY_DOWN)) for of in range(2)]

    @pl.when(core == 1)
    def _():
        for part in late_parts:
            pass_late(*part).start()

    def far_pieces(first, last):
        @pl.loop(first, last)
        def _(j):
            copy_to(far_chip, 2 * j, send.at[2], far_a.at[j], to_up).wait_recv()
            to_partner(far, 2 * j)
            copy_to(far_chip, 2 * j + 1, send.at[3], far_b.at[j], to_down).wait_recv()
            to_partner(far, 2 * j + 1)

    far_pieces(1, 6)

    @pl.when(z != 0)
    def _():
        gz_copy(z, to_zero).wait_send()
        nz_back(1).wait_recv()

    @pl.when(z == 0)
    def _():
        for i in range(1, 4):
            nz_back(i).wait_send()

    nz_part.start()
    far_pieces(6, 9)
    nz_part.wait()

    def all_of(src, count, send_sem, recv_sem, to):
        part = b.at[src, pl.ds(0, count)]
        return pltpu.make_async_remote_copy(
            src_ref=part, dst_ref=part, send_sem=send_sem, recv_sem=recv_sem,
            device_id=to, device_id_type=MESH,
        )

    all_of(rows, PIECES, send.at[0], near_a.at[0], to_up).wait_send()
    all_of(rows, PIECES, send.at[1], near_b.at[0], to_down).wait_send()
    all_of(rows, 8, send.at[2], far_a.at[0], to_up).wait_send()
    all_of(rows, 8, send.at[3], far_b.at[0], to_down).wait_send()
    for chip, count in ((z, PIECES), (up, PIECES - 2), (down, PIECES - 2), (far, PIECES - 2)):
        all_of(chip * 2 + core, count, part_send.at[chip], part_recv.at[chip], to_part).wait_send()
        all_of(chip * 2 + 1 - core, count, part_send.at[chip], part_recv.at[chip], to_part).wait_recv()

    @pl.when(core == 1)
    def _():
        for part in late_parts:
            pass_late(*part).wait()


def comm(*args):
    bf16, f32 = jnp.bfloat16, jnp.float32
    dma = pltpu.SemaphoreType.DMA
    return pl.pallas_call(
        comm_kernel,
        out_shape=[
            pltpu.VMEM((8, PIECES, 128, 512), bf16), pltpu.VMEM((2, 2, 128, 512), bf16),
            pltpu.VMEM((2, 4, 8, 128), f32),
        ],
        in_specs=[HBM] * len(args),
        out_specs=[VMEM] * 3,
        scratch_shapes=[
            pltpu.VMEM((1024, 512), bf16), pltpu.VMEM((64, 1024), bf16), pltpu.VMEM((64, 1024), bf16),
            pltpu.VMEM((512, 1024), bf16),
            pltpu.VMEM((16, 1024), bf16), pltpu.VMEM((16, 512), bf16),
            pltpu.VMEM((16, 1024), bf16), pltpu.VMEM((16, 64), bf16),
            pltpu.VMEM((16, 1024), bf16), pltpu.VMEM((16, 64), bf16),
            pltpu.VMEM((16, 512), bf16), pltpu.VMEM((16, 1024), bf16),
            pltpu.VMEM((1, 64), f32), pltpu.VMEM((1, 64), f32),
            pltpu.VMEM((4, 1, 128), f32), pltpu.VMEM((4, 4, 128), f32), pltpu.VMEM((4, 2, 4, 128), f32),
            dma((14,)), dma((4,)), dma((PIECES,)), dma((PIECES,)), dma((PIECES // 2,)), dma((PIECES // 2,)),
            dma((4,)), dma((4,)),
            dma, dma((4,)), dma((3,)), dma((3,)), dma((3,)), dma((3,)), dma((4,)), dma((4,)),
            dma((2, 2, 2)), dma((2, 2, 2)), dma((4, 2)), dma((4, 2)),
        ],
        compiler_params=pltpu.CompilerParams(
            collective_id=0, has_side_effects=True, vmem_limit_bytes=44 * 2**20
        ),
        name="comm",
    )(*args)


def put_narrow(r, block, k, v, sem):
    for i, out in enumerate((k, v)):
        for j in range(2):
            cols = pl.ds(pl.multiple_of(r * 1024 + j * 512, 512), 512)
            pltpu.make_async_copy(block.at[i, pl.ds(j * 64, 64)], out.at[:, cols], sem.at[i]).start()


def write_kernel(b, late, nz, q, k, v, m, n, gain, sem):
    tiles = [nz[r % 2, r // 2] for r in range(8)]
    gain[...] = jnp.concatenate(tiles, axis=0).astype(jnp.bfloat16)
    for r in range(8):
        pltpu.make_async_copy(b.at[r, pl.ds(10, 8)], m.at[pl.ds(r * 8, 8)], sem.at[3]).start()
        for j in range(2):
            cols = pl.ds(r * 1024 + j * 512, 512)
            pltpu.make_async_copy(b.at[r, pl.ds(2 + 4 * j, 4)], q.at[:, :, cols], sem.at[2]).start()
    rows = lax.axis_index("rows")
    core = rows % 2
    far = (rows // 2 + 2) % 4 * 2
    for d in range(2, 8):
        r = (far + d) % 8
        put_narrow(r, b.at[r, pl.ds(0, 2)], k, v, sem)
    pltpu.make_async_copy(gain, n, sem.at[4]).start()

    def wait(i, ref):
        pltpu.make_async_copy(ref, ref, sem.at[i]).wait()

    @pl.when(core == 1)
    def _():
        for of in range(2):
            put_narrow(far + of, late.at[of], k, v, sem)
        wait(0, k)
        wait(1, v)

    @pl.when(core == 0)
    def _():
        wait(0, k.at[:, pl.ds(0, 6144)])
        wait(1, v.at[:, pl.ds(0, 6144)])

    for i, ref in ((2, q), (3, m), (4, n)):
        wait(i, ref)


def write(b, late, nz):
    bf16 = jnp.bfloat16
    shapes = [(4, 128, 8192), (64, 8192), (64, 8192), (64, 128, 512), (64, 128)]
    return pl.pallas_call(
        write_kernel,
        out_shape=[jax.ShapeDtypeStruct(s, bf16) for s in shapes],
        in_specs=[VMEM] * 3,
        out_specs=[HBM] * 5,
        scratch_shapes=[pltpu.VMEM((64, 128), bf16), pltpu.SemaphoreType.DMA((5,))],
        compiler_params=pltpu.CompilerParams(vmem_limit_bytes=4 * 2**20),
        cost_estimate=pl.CostEstimate(flops=0, bytes_accessed=38 * 2**20, transcendentals=0),
        name="write",
    )(b, late, nz)


def last_kernel(other, k_in, v_in, k, v, sem):
    rows = lax.axis_index("rows")
    far = (rows // 2 + 2) % 4 * 2

    @pl.when(rows % 2 == 0)
    def _():
        for of in range(2):
            put_narrow(far + of, other.at[of], k, v, sem)
        for i, ref in enumerate((k, v)):
            part = ref.at[:, pl.ds(0, 2048)]
            pltpu.make_async_copy(part, part, sem.at[i]).wait()


def write_last(other, k, v):
    return pl.pallas_call(
        last_kernel,
        out_shape=[jax.ShapeDtypeStruct(a.shape, a.dtype) for a in (k, v)],
        in_specs=[VMEM, HBM, HBM],
        out_specs=[HBM] * 2,
        scratch_shapes=[pltpu.SemaphoreType.DMA((2,))],
        input_output_aliases={1: 0, 2: 1},
        compiler_params=pltpu.CompilerParams(vmem_limit_bytes=2**20),
        name="write_last",
    )(other, k, v)


def body(
    train_query, low_query, high_query, train_key, low_key, high_key, train_value, low_value, high_value,
    train_mixed, low_mixed, high_mixed, norm_train, norm_step,
):
    b, late, nz = comm(
        train_query, train_key.T, train_value.T, train_mixed,
        low_query.T, high_query, low_key.T, high_key, low_value.T, high_value, low_mixed.T, high_mixed,
        norm_train.reshape(1, 64), norm_step.reshape(1, 64),
    )
    other = lax.ppermute(late, "rows", [(r, r + 1 - 2 * (r % 2)) for r in range(8)])
    q, k, v, m, n = write(b, late, nz)
    k, v = write_last(other, k, v)
    return q.reshape(512, 8192), k, v, m.reshape(8192, 512), n.reshape(8192)


def solution(mesh):
    R, M = "rows", "model"
    return jax.shard_map(
        body,
        mesh=mesh,
        in_specs=(
            P(R, M), P(R, None), P(None, M),
            P(R, M), P(R, None), P(None, M),
            P(R, M), P(R, None), P(None, M),
            P(M, R), P(M, None), P(None, R),
            P((R, M)), P((R, M)),
        ),
        out_specs=(P(M, None), P(M, None), P(M, None), P(None, M), P()),
        check_vma=False,
    )
```

```python
import jax
import jax.numpy as jnp
from jax import lax
from jax.experimental import pallas as pl
from jax.experimental.pallas import tpu as pltpu
from jax.sharding import PartitionSpec as P

MESH = pl.DeviceIdType.MESH
HBM = pl.BlockSpec(memory_space=pltpu.HBM)
VMEM = pl.BlockSpec(memory_space=pltpu.VMEM)

mix_rate = 0.5

PIECES = 18

SPLIT = 112
WAY_UP = ((0, 0, SPLIT),)
WAY_DOWN = ((0, SPLIT, 128 - SPLIT), (1, 0, 128)) if SPLIT < 128 else ((1, 0, 128),)


def comm_kernel(
    tq, tk, tv, tm, lq, hq, lk, hk, lv, hv, lm, hm, na, nb,
    b, late, nz,
    xq, xk, xv, xm, slq, shq, slk, shk, slv, shv, slm, shm, sna, snb, gz, gx, gy,
    ld, send, near_a, near_b, far_a, far_b, part_send, part_recv,
    gz_send, gz_recv, gx_send, gx_recv, gy_send, gy_recv, nz_send, nz_recv,
    late_send, late_recv, early_send, early_recv,
):
    rows = lax.axis_index("rows")
    model = lax.axis_index("model")
    z, core = rows // 2, rows % 2
    y, x = model // 4, model % 4
    up, down = (z + 1) % 4, (z + 3) % 4
    far = (z + 2) % 4
    right, left, above, below = (x + 1) % 4, (x + 3) % 4, (y + 1) % 4, (y + 3) % 4
    to_up = {"rows": up * 2 + core}
    to_down = {"rows": down * 2 + core}
    to_part = {"rows": z * 2 + 1 - core}
    to_far, to_zero = {"rows": far * 2 + core}, {"rows": core}
    to_right, to_left = {"model": y * 4 + right}, {"model": y * 4 + left}
    to_above, to_below = {"model": above * 4 + x}, {"model": below * 4 + x}

    barrier = pltpu.get_barrier_semaphore()
    for peer in (to_up, to_down, to_part):
        pl.semaphore_signal(barrier, inc=1, device_id=peer, device_id_type=MESH)

    @pl.when(z == 0)
    def _():
        for peer in (to_far, to_right, to_left, to_above, to_below):
            pl.semaphore_signal(barrier, inc=1, device_id=peer, device_id_type=MESH)

    @pl.when(z == 2)
    def _():
        pl.semaphore_signal(barrier, inc=1, device_id=to_far, device_id_type=MESH)

    loads = [
        (tk, xk), (lk, slk), (hk, shk), (na, sna), (nb, snb), (tv, xv), (lv, slv), (hv, shv),
        (lm, slm), (hm, shm), (tm, xm),
        (lq, slq), (hq, shq), (tq, xq),
    ]
    loads = [pltpu.make_async_copy(s, d, ld.at[i]) for i, (s, d) in enumerate(loads)]
    for c in loads:
        c.start()

    def low_rank(high, low):
        return mix_rate * lax.dot_general(
            high, low, (((0,), (0,)), ((), ())), preferred_element_type=jnp.float32
        )

    def make_narrow(k, base, high, low):
        for j in range(2):
            cols = pl.ds(j * 512, 512)
            b[rows, k, pl.ds(j * 64, 64), :] = (
                base[:, cols].astype(jnp.float32) + low_rank(high[...], low[:, cols])
            ).astype(jnp.bfloat16)

    def copy_to(src, index, send_sem, recv_sem, to):
        return pltpu.make_async_remote_copy(
            src_ref=b.at[src, index], dst_ref=b.at[src, index], send_sem=send_sem,
            recv_sem=recv_sem, device_id=to, device_id_type=MESH,
        )

    def gz_copy(chip, to):
        return pltpu.make_async_remote_copy(
            src_ref=gz.at[chip], dst_ref=gz.at[chip], send_sem=gz_send, recv_sem=gz_recv.at[chip],
            device_id=to, device_id_type=MESH,
        )

    def send_own(k):
        copy_to(rows, k, send.at[0], near_a.at[k], to_up).start()
        copy_to(rows, k, send.at[1], near_b.at[k], to_down).start()

    def to_partner(chip, k):
        copy_to(chip * 2 + core, k, part_send.at[chip], part_recv.at[chip], to_part).start()

    def early(chip, k):
        return copy_to(chip * 2 + core, k, early_send.at[chip, k], early_recv.at[chip, k], to_part)

    for c in loads[:5]:
        c.wait()
    gain = sna[...] + snb[...]
    gz[z] = jnp.concatenate([gain, gain], axis=1)
    make_narrow(0, xk, shk, slk)
    pl.when(z == 0)(lambda: pl.semaphore_wait(barrier, 8))
    pl.when(z == 2)(lambda: pl.semaphore_wait(barrier, 4))
    pl.when(z % 2 == 1)(lambda: pl.semaphore_wait(barrier, 3))

    @pl.when(z != 0)
    def _():
        gz_copy(z, to_zero).start()

    for c in loads[5:8]:
        c.wait()
    send_own(0)
    make_narrow(1, xv, shv, slv)
    for c in loads[8:]:
        c.wait()
    send_own(1)
    to_partner(z, 0)
    to_partner(z, 1)

    def make_query(i):
        left, top = (i // 4) * 512, (i % 4) * 128
        left, top = pl.multiple_of(left, 512), pl.multiple_of(top, 128)
        part = low_rank(shq[:, pl.ds(top, 128)], slq[:, pl.ds(left, 512)])
        base = xq[pl.ds(left, 512), pl.ds(top, 128)].astype(jnp.float32)
        b[rows, 2 + i] = (base.T + part).astype(jnp.bfloat16)

    def make_mixed(i):
        top = pl.multiple_of(i * 128, 128)
        part = low_rank(shm[:, pl.ds(top, 128)], slm[...])
        base = xm[:, pl.ds(top, 128)].astype(jnp.float32)
        b[rows, 10 + i] = (base.T + part).astype(jnp.bfloat16)

    make_query(0)

    @pl.loop(1, 8)
    def _(i):
        make_query(i)
        send_own(1 + i)
        to_partner(z, 1 + i)

    make_mixed(0)
    send_own(9)
    to_partner(z, 9)

    @pl.loop(1, 8)
    def _(i):
        make_mixed(i)
        send_own(9 + i)
        to_partner(z, 9 + i)

    def tile(ref, src, sems, k, to):
        return pltpu.make_async_remote_copy(
            src_ref=ref.at[src], dst_ref=ref.at[src], send_sem=sems[0].at[k], recv_sem=sems[1].at[k],
            device_id=to, device_id_type=MESH,
        )

    def both(ref, src, sems, one, other):
        return [tile(ref, src, sems, 0, one), tile(ref, src, sems, 1, other)]

    gx_sems, gy_sems, nz_sems = (gx_send, gx_recv), (gy_send, gy_recv), (nz_send, nz_recv)
    gx_near, gx_far = both(gx, x, gx_sems, to_right, to_left), tile(gx, left, gx_sems, 2, to_right)
    gy_near, gy_far = both(gy, y, gy_sems, to_above, to_below), tile(gy, below, gy_sems, 2, to_above)
    nz_part = tile(nz, core, nz_sems, 3, to_part)

    def nz_back(chip):
        return pltpu.make_async_remote_copy(
            src_ref=nz.at[core], dst_ref=nz.at[core], send_sem=nz_send.at[chip - 1], recv_sem=nz_recv.at[0],
            device_id={"rows": chip * 2 + core}, device_id_type=MESH,
        )

    def make_x():
        for i in range(1, 4):
            gz_copy(i, to_up).wait_recv()
        for i in range(4):
            gx[x, i : i + 1] = gz[i]

    def near_x():
        for c in gx_near:
            c.start()

    def far_x():
        for c in gx_near:
            c.wait()
        gx_far.start()

    def make_y():
        gx_far.wait()
        lane = lax.broadcasted_iota(jnp.int32, (4, 128), 1)
        gy[y, 0] = jnp.where(lane < 64, gx[0], gx[1])
        gy[y, 1] = jnp.where(lane < 64, gx[2], gx[3])

    def near_y():
        for c in gy_near:
            c.start()

    def far_y():
        for c in gy_near:
            c.wait()
        gy_far.start()

    def make_z():
        gy_far.wait()
        for i in range(4):
            for k in range(8):
                nz[core, i, k : k + 1] = gy[k // 2, k % 2, i : i + 1]

    def back_z():
        for i in range(1, 4):
            nz_back(i).start()

    gain_steps = [near_x, far_x, make_y, near_y, far_y, make_z, back_z]
    pl.when(z == 0)(make_x)
    send_own(17)
    to_partner(z, 17)

    def pass_on(k, src):
        way, sem, to = ((2, far_a, to_up), (3, far_b, to_down))[k % 2]
        return copy_to(src, k, send.at[way], sem.at[k // 2], to)

    def pass_late(way, n, of):
        (piece, first, count), to = ((WAY_UP, WAY_DOWN)[way][n], (to_up, to_down)[way])
        some = pl.ds(first, count)
        return pltpu.make_async_remote_copy(
            src_ref=b.at[(down, up)[way] * 2 + of, piece, some], dst_ref=late.at[of, piece, some],
            send_sem=late_send.at[of, way, n], recv_sem=late_recv.at[of, way, n], device_id=to, device_id_type=MESH,
        )

    below_chip, above_chip = down * 2 + core, up * 2 + core
    far_chip = far * 2 + core
    for k in range(PIECES):
        copy_to(below_chip, k, send.at[0], near_a.at[k], to_up).wait_recv()
        if k >= 2 and k % 2 == 0:
            pass_on(k, below_chip).start()
        early(down, k).start() if k < 2 else to_partner(down, k)
        copy_to(above_chip, k, send.at[1], near_b.at[k], to_down).wait_recv()
        if k >= 2 and k % 2 == 1:
            pass_on(k, above_chip).start()
        early(up, k).start() if k < 2 else to_partner(up, k)
        if k < len(gain_steps):
            pl.when(z == 0)(gain_steps[k])

    for chip in (down, up):
        for k in range(2):
            early(chip, k).wait()
    late_parts = [(0, n, of) for n in range(len(WAY_UP)) for of in range(2)]
    late_parts += [(1, n, of) for n in range(len(WAY_DOWN)) for of in range(2)]

    @pl.when(core == 1)
    def _():
        for part in late_parts:
            pass_late(*part).start()

    def far_pieces(first, last):
        @pl.loop(first, last)
        def _(j):
            copy_to(far_chip, 2 * j, send.at[2], far_a.at[j], to_up).wait_recv()
            to_partner(far, 2 * j)
            copy_to(far_chip, 2 * j + 1, send.at[3], far_b.at[j], to_down).wait_recv()
            to_partner(far, 2 * j + 1)

    far_pieces(1, 6)

    @pl.when(z != 0)
    def _():
        gz_copy(z, to_zero).wait_send()
        nz_back(1).wait_recv()

    @pl.when(z == 0)
    def _():
        for i in range(1, 4):
            nz_back(i).wait_send()

    nz_part.start()
    far_pieces(6, 9)
    nz_part.wait()

    def all_of(src, count, send_sem, recv_sem, to):
        part = b.at[src, pl.ds(0, count)]
        return pltpu.make_async_remote_copy(
            src_ref=part, dst_ref=part, send_sem=send_sem, recv_sem=recv_sem,
            device_id=to, device_id_type=MESH,
        )

    all_of(rows, PIECES, send.at[0], near_a.at[0], to_up).wait_send()
    all_of(rows, PIECES, send.at[1], near_b.at[0], to_down).wait_send()
    all_of(rows, 8, send.at[2], far_a.at[0], to_up).wait_send()
    all_of(rows, 8, send.at[3], far_b.at[0], to_down).wait_send()
    for chip, count in ((z, PIECES), (up, PIECES - 2), (down, PIECES - 2), (far, PIECES - 2)):
        all_of(chip * 2 + core, count, part_send.at[chip], part_recv.at[chip], to_part).wait_send()
        all_of(chip * 2 + 1 - core, count, part_send.at[chip], part_recv.at[chip], to_part).wait_recv()

    @pl.when(core == 1)
    def _():
        for part in late_parts:
            pass_late(*part).wait()


def comm(*args):
    bf16, f32 = jnp.bfloat16, jnp.float32
    dma = pltpu.SemaphoreType.DMA
    return pl.pallas_call(
        comm_kernel,
        out_shape=[
            pltpu.VMEM((8, PIECES, 128, 512), bf16), pltpu.VMEM((2, 2, 128, 512), bf16),
            pltpu.VMEM((2, 4, 8, 128), f32),
        ],
        in_specs=[HBM] * len(args),
        out_specs=[VMEM] * 3,
        scratch_shapes=[
            pltpu.VMEM((1024, 512), bf16), pltpu.VMEM((64, 1024), bf16), pltpu.VMEM((64, 1024), bf16),
            pltpu.VMEM((512, 1024), bf16),
            pltpu.VMEM((16, 1024), bf16), pltpu.VMEM((16, 512), bf16),
            pltpu.VMEM((16, 1024), bf16), pltpu.VMEM((16, 64), bf16),
            pltpu.VMEM((16, 1024), bf16), pltpu.VMEM((16, 64), bf16),
            pltpu.VMEM((16, 512), bf16), pltpu.VMEM((16, 1024), bf16),
            pltpu.VMEM((1, 64), f32), pltpu.VMEM((1, 64), f32),
            pltpu.VMEM((4, 1, 128), f32), pltpu.VMEM((4, 4, 128), f32), pltpu.VMEM((4, 2, 4, 128), f32),
            dma((14,)), dma((4,)), dma((PIECES,)), dma((PIECES,)), dma((PIECES // 2,)), dma((PIECES // 2,)),
            dma((4,)), dma((4,)),
            dma, dma((4,)), dma((3,)), dma((3,)), dma((3,)), dma((3,)), dma((4,)), dma((4,)),
            dma((2, 2, 2)), dma((2, 2, 2)), dma((4, 2)), dma((4, 2)),
        ],
        compiler_params=pltpu.CompilerParams(
            collective_id=0, has_side_effects=True, vmem_limit_bytes=44 * 2**20
        ),
        name="comm",
    )(*args)


def put_narrow(r, block, k, v, sem):
    for i, out in enumerate((k, v)):
        for j in range(2):
            cols = pl.ds(pl.multiple_of(r * 1024 + j * 512, 512), 512)
            pltpu.make_async_copy(block.at[i, pl.ds(j * 64, 64)], out.at[:, cols], sem.at[i]).start()


def write_kernel(b, late, nz, q, k, v, m, n, gain, sem):
    for r in range(8):
        pltpu.make_async_copy(b.at[r, pl.ds(10, 8)], m.at[pl.ds(r * 8, 8)], sem.at[3]).start()
        for j in range(2):
            cols = pl.ds(r * 1024 + j * 512, 512)
            pltpu.make_async_copy(b.at[r, pl.ds(2 + 4 * j, 4)], q.at[:, :, cols], sem.at[2]).start()
    tiles = [nz[r % 2, r // 2] for r in range(8)]
    gain[...] = jnp.concatenate(tiles, axis=0).astype(jnp.bfloat16)
    rows = lax.axis_index("rows")
    core = rows % 2
    far = (rows // 2 + 2) % 4 * 2
    for d in range(2, 8):
        r = (far + d) % 8
        put_narrow(r, b.at[r, pl.ds(0, 2)], k, v, sem)
    pltpu.make_async_copy(gain, n, sem.at[4]).start()

    def wait(i, ref):
        pltpu.make_async_copy(ref, ref, sem.at[i]).wait()

    @pl.when(core == 1)
    def _():
        for of in range(2):
            put_narrow(far + of, late.at[of], k, v, sem)
        wait(0, k)
        wait(1, v)

    @pl.when(core == 0)
    def _():
        wait(0, k.at[:, pl.ds(0, 6144)])
        wait(1, v.at[:, pl.ds(0, 6144)])

    for i, ref in ((2, q), (3, m), (4, n)):
        wait(i, ref)


def write(b, late, nz):
    bf16 = jnp.bfloat16
    shapes = [(4, 128, 8192), (64, 8192), (64, 8192), (64, 128, 512), (64, 128)]
    return pl.pallas_call(
        write_kernel,
        out_shape=[jax.ShapeDtypeStruct(s, bf16) for s in shapes],
        in_specs=[VMEM] * 3,
        out_specs=[HBM] * 5,
        scratch_shapes=[pltpu.VMEM((64, 128), bf16), pltpu.SemaphoreType.DMA((5,))],
        compiler_params=pltpu.CompilerParams(vmem_limit_bytes=4 * 2**20),
        cost_estimate=pl.CostEstimate(flops=0, bytes_accessed=38 * 2**20, transcendentals=0),
        name="write",
    )(b, late, nz)


def last_kernel(other, k_in, v_in, k, v, sem):
    rows = lax.axis_index("rows")
    far = (rows // 2 + 2) % 4 * 2

    @pl.when(rows % 2 == 0)
    def _():
        for of in range(2):
            put_narrow(far + of, other.at[of], k, v, sem)
        for i, ref in enumerate((k, v)):
            part = ref.at[:, pl.ds(0, 2048)]
            pltpu.make_async_copy(part, part, sem.at[i]).wait()


def write_last(other, k, v):
    return pl.pallas_call(
        last_kernel,
        out_shape=[jax.ShapeDtypeStruct(a.shape, a.dtype) for a in (k, v)],
        in_specs=[VMEM, HBM, HBM],
        out_specs=[HBM] * 2,
        scratch_shapes=[pltpu.SemaphoreType.DMA((2,))],
        input_output_aliases={1: 0, 2: 1},
        compiler_params=pltpu.CompilerParams(vmem_limit_bytes=2**20),
        name="write_last",
    )(other, k, v)


def body(
    train_query, low_query, high_query, train_key, low_key, high_key, train_value, low_value, high_value,
    train_mixed, low_mixed, high_mixed, norm_train, norm_step,
):
    b, late, nz = comm(
        train_query, train_key.T, train_value.T, train_mixed,
        low_query.T, high_query, low_key.T, high_key, low_value.T, high_value, low_mixed.T, high_mixed,
        norm_train.reshape(1, 64), norm_step.reshape(1, 64),
    )
    other = lax.ppermute(late, "rows", [(r, r + 1 - 2 * (r % 2)) for r in range(8)])
    q, k, v, m, n = write(b, late, nz)
    k, v = write_last(other, k, v)
    return q.reshape(512, 8192), k, v, m.reshape(8192, 512), n.reshape(8192)


def solution(mesh):
    R, M = "rows", "model"
    return jax.shard_map(
        body,
        mesh=mesh,
        in_specs=(
            P(R, M), P(R, None), P(None, M),
            P(R, M), P(R, None), P(None, M),
            P(R, M), P(R, None), P(None, M),
            P(M, R), P(M, None), P(None, R),
            P((R, M)), P((R, M)),
        ),
        out_specs=(P(M, None), P(M, None), P(M, None), P(None, M), P()),
        check_vma=False,
    )
```
